32 devices in a mesh: batch: 4 (over z), seq: 8 (over y, x, core).
Axes of the slice: x: 2, y: 2, z: 4, core: 2. Of those that a mesh axis runs over, the one named last changes fastest.
Arguments:
- tokens: bfloat16 [10240, 8192], P(('batch', 'seq')), may hold values from -6 to 6
- out_grad: bfloat16 [10240, 8192], P(('batch', 'seq')), may hold values from -0.109375 to 0.109375
- gate_pre: bfloat16 [10240, 768], P(('batch', 'seq')), may hold values from -8 to 8
- up_pre: bfloat16 [10240, 768], P(('batch', 'seq')), may hold values from -6 to 6
- hidden_grad: bfloat16 [10240, 768], P(('batch', 'seq')), may hold values from -0.0625 to 0.0625
Outputs:
- gate_weight_grad: float32 [8192, 768], P(('seq', 'batch'))
- up_weight_grad: float32 [8192, 768], P(('seq', 'batch'))
- down_weight_grad: float32 [8192, 768], P(('seq', 'batch'))
The draws below stay inside these ranges and needn't reach their ends.
All inputs are finite; a program needn't handle non-finite values.
Results may differ from the reference program's by a relative error of at most 0.019.
Values may be sent and summed in bfloat16 or wider, within the bound.
A program may use at most 192 MiB of HBM per device.

```python
import jax
import jax.numpy as jnp
from jax import lax

D = 8192
FF = 768
TOK_DEV = 320
TOKENS = 10240
N_BATCH = 4
N_SEQ = 8


def strengthened(result, stream_key, source, target, blocks, factor):
    owner, partner = [(jnp.arange(result.shape[position]) // (result.shape[position] // blocks)).reshape([-1 if axis == position else 1 for axis in range(result.ndim)]) for position in (source, target)]
    chosen = jax.random.permutation(stream_key, blocks)[partner]
    strong = (owner == chosen) | (owner == (partner + blocks // 2) % blocks)
    return jnp.where(strong, factor * result, result)


def shard_levels(rng, shape, cuts, smallest, top_value):
    factor_of, own = 1.0, jax.random.fold_in(rng, 6)
    for position, blocks in cuts:
        steps = jnp.exp(jax.random.uniform(jax.random.fold_in(own, position), (blocks,), jnp.float32, smallest / len(cuts), top_value / len(cuts)))
        factor_of = factor_of * jnp.repeat(steps, shape[position] // blocks).reshape([-1 if axis == position else 1 for axis in range(len(shape))])
    return factor_of


def gaussian(own_key, extent, deviation, reach, split=(), kind=jnp.bfloat16):
    array = deviation * jax.random.normal(own_key, extent, jnp.float32)
    if split:
        array = array * shard_levels(own_key, extent, split, -0.22, 0.18)
    return jnp.clip(array, -reach, reach).astype(kind)


def heavy_noise(own_key, extent, width, most, split, heavy, kind=jnp.bfloat16):
    entries = width * jax.random.normal(own_key, extent, jnp.float32)
    if split:
        entries = entries * shard_levels(own_key, extent, split, -0.22, 0.18)
    return jnp.clip(strengthened(entries, jax.random.fold_in(own_key, 3), *heavy), -most, most).astype(kind)


def setup_inputs(seed: int = 0) -> dict:
    key_of = jax.random.split(jax.random.key(seed), 6)
    tokens = heavy_noise(key_of[0], (TOKENS, D), 1.0, 6.0, ((0, 32),), (0, 1, 32, 2.75))
    out_grad = heavy_noise(key_of[1], (TOKENS, D), TOKENS ** -0.5, 0.109375, ((0, 32),), (0, 1, 32, 2.75))
    gate_pre = gaussian(key_of[2], (TOKENS, FF), 1.5, 8.0, ((0, 32),))
    up_pre = gaussian(key_of[3], (TOKENS, FF), 1.0, 6.0, ((0, 32),))
    hidden_grad = gaussian(key_of[4], (TOKENS, FF), TOKENS ** -0.5, 0.0625, ((0, 32),))
    return {"tokens": tokens, "out_grad": out_grad, "gate_pre": gate_pre, "up_pre": up_pre, "hidden_grad": hidden_grad}


def hidden_parts(gate_pre, up_pre, hidden_grad):
    gate_val = gate_pre.astype(jnp.float32)
    up_val = up_pre.astype(jnp.float32)
    grad_val = hidden_grad.astype(jnp.float32)
    sigmoid_val = jax.nn.sigmoid(gate_val)
    activated = gate_val * sigmoid_val
    hidden = (activated * up_val).astype(jnp.bfloat16)
    up_cotangent = (grad_val * activated).astype(jnp.bfloat16)
    gate_cotangent = (grad_val * up_val * sigmoid_val * (1.0 + gate_val * (1.0 - sigmoid_val))).astype(jnp.bfloat16)
    return hidden, gate_cotangent, up_cotangent


def contract_rows(left, right):
    return lax.dot_general(left, right, (((0,), (0,)), ((), ())), preferred_element_type=jnp.float32)


def reference(tokens, out_grad, gate_pre, up_pre, hidden_grad):
    hidden, gate_cotangent, up_cotangent = hidden_parts(gate_pre, up_pre, hidden_grad)
    cotangents = jnp.concatenate([gate_cotangent, up_cotangent], axis=1)
    blocks = N_BATCH * N_SEQ
    model_width = tokens.shape[1]
    hidden_width = hidden.shape[1]

    def add_block(total, pieces):
        features, grads, cotangent_rows, hidden_slice = pieces
        term = jnp.concatenate([contract_rows(features, cotangent_rows), contract_rows(grads, hidden_slice)], axis=1)
        return total + lax.optimization_barrier(term.astype(jnp.bfloat16)).astype(jnp.float32), None

    pieces = (tokens.reshape(blocks, TOK_DEV, model_width), out_grad.reshape(blocks, TOK_DEV, model_width),
              cotangents.reshape(blocks, TOK_DEV, 2 * hidden_width), hidden.reshape(blocks, TOK_DEV, hidden_width))
    total, unused = lax.scan(add_block, jnp.zeros((model_width, 3 * hidden_width), jnp.float32), pieces)
    return (total[:, :hidden_width], total[:, hidden_width:2 * hidden_width], total[:, 2 * hidden_width:])
```

```python
import functools

import jax
import jax.numpy as jnp
from jax import lax
from jax.experimental import pallas as pl
from jax.experimental.pallas import tpu as pltpu
from jax.sharding import PartitionSpec as P

MESH = pl.DeviceIdType.MESH
LANES = 128


def bit_count(n):
    return n.bit_length() - 1


def flip(value, mask):
    out, bit = value, 1
    while bit <= mask:
        if mask & bit:
            out = out + bit * (1 - 2 * ((value // bit) % 2))
        bit *= 2
    return out


class Plan:
    def __init__(self, n_batch, n_seq, tok, width, hidden):
        self.n_batch, self.n_seq, self.tok, self.width, self.hidden = n_batch, n_seq, tok, width, hidden
        self.chips = n_seq // 2
        self.seq_bits, self.batch_bits = bit_count(self.chips), bit_count(n_batch)
        self.rows = width // (n_batch * n_seq)
        self.group = max(1, LANES // self.rows)
        self.block = self.group * self.rows
        self.n_groups = n_batch // self.group
        total = 3 * hidden
        units = total // LANES
        late = max(2, units // 6)
        early = (units - late) // 2
        cuts = [0, early, units - late, units - late // 2, units]
        self.spans = [(a * LANES, b * LANES) for a, b in zip(cuts[:-1], cuts[1:])]
        self.ascending = [True, False, True, False]
        self.batch_first = [False, False, True, True]

    def seq_bit(self, cls, stage):
        return stage if self.ascending[cls] else self.seq_bits - 1 - stage

    def position(self, cls, u):
        if not self.ascending[cls]:
            return u
        return sum(((u // (1 << i)) % 2) * (1 << (self.seq_bits - 1 - i)) for i in range(self.seq_bits))

    def pieces(self, lo, hi, step):
        out = []
        while lo < hi:
            end = min(hi, (lo // step + 1) * step)
            out.append((lo, end))
            lo = end
        return out


def low_bit(m):
    return (m & -m).bit_length() - 1


def kernel(plan, tokens, out_grad, gate_pre, up_pre, hidden_grad, out_gate, out_up, out_down, *scratch):
    p = plan
    T, R, M, C, NB = p.tok, p.rows, p.block, p.chips, p.n_batch
    n_cls, sb, bb = len(p.spans), p.seq_bits, p.batch_bits
    scratch = list(scratch)
    raw, hid, tok_v, grad_v = (scratch.pop(0) for _ in range(4))
    terms = [scratch.pop(0) for _ in range(n_cls)]
    seq_in = [[scratch.pop(0) for _ in range(sb)] for _ in range(n_cls)]
    batch_in = [[scratch.pop(0) for _ in range(bb)] for _ in range(n_cls)]
    raw_sem, load_sem, swap_sem, swap_out, seq_send, seq_recv, batch_send, batch_recv = scratch
    outs = (out_gate, out_up, out_down)

    b_me, s_me = lax.axis_index("batch"), lax.axis_index("seq")
    core, chip = s_me % 2, s_me // 2
    twin = (b_me, s_me + 1 - 2 * core)
    seq_peer = [(b_me, flip(s_me, 2 << i)) for i in range(sb)]
    batch_peer = [(flip(b_me, 1 << i), s_me) for i in range(bb)]

    pre = (gate_pre, up_pre, hidden_grad)
    for i, ref in enumerate(pre):
        pltpu.make_async_copy(ref, raw.at[i, pl.ds(0, T)], raw_sem.at[0]).start()

    def column(g, u, side):
        k = flip(chip, u)
        first = flip(b_me // p.group, g) * p.group
        return pl.multiple_of(((k * 2 + side) * NB + first) * R, M)

    sends = []
    groups = list(range(p.n_groups - 1, -1, -1))

    def load(g):
        for a, (src, dst) in enumerate(((tokens, tok_v), (out_grad, grad_v))):
            for u in range(C):
                pltpu.make_async_copy(
                    src.at[:, pl.ds(column(g, u, core), M)], dst.at[g, u, pl.ds(0, T)], load_sem.at[g, a]
                ).start()

    def swap(g):
        for a, (src, dst) in enumerate(((tokens, tok_v), (out_grad, grad_v))):
            for u in range(C):
                pltpu.make_async_remote_copy(
                    src_ref=src.at[:, pl.ds(column(g, u, 1 - core), M)],
                    dst_ref=dst.at[g, u, pl.ds(T, T)],
                    send_sem=swap_out.at[g, a],
                    recv_sem=swap_sem.at[g, a],
                    device_id=twin,
                    device_id_type=MESH,
                ).start()

    for g in groups:
        load(g)

    barrier = pltpu.get_barrier_semaphore()
    peers = [twin] + seq_peer + batch_peer
    for peer in peers:
        pl.semaphore_signal(barrier, inc=1, device_id=peer, device_id_type=MESH)
    pl.semaphore_wait(barrier, len(peers))

    for i, ref in enumerate(pre):
        pltpu.make_async_remote_copy(
            src_ref=ref, dst_ref=raw.at[i, pl.ds(T, T)], send_sem=raw_sem.at[1], recv_sem=raw_sem.at[2],
            device_id=twin, device_id_type=MESH,
        ).start()
    for g in groups:
        swap(g)

    def activate(side):
        step = 32
        def body(i, carry):
            at = pl.ds(pl.multiple_of(side * T + i * step, step), step)
            gate_val = raw[0, at, :].astype(jnp.float32)
            up_val = raw[1, at, :].astype(jnp.float32)
            grad_val = raw[2, at, :].astype(jnp.float32)
            sig = jax.nn.sigmoid(gate_val)
            act = gate_val * sig
            F = p.hidden
            hid[at, 0:F] = (grad_val * up_val * sig * (1.0 + gate_val * (1.0 - sig))).astype(jnp.bfloat16)
            hid[at, F:2 * F] = (grad_val * act).astype(jnp.bfloat16)
            hid[at, 2 * F:3 * F] = (act * up_val).astype(jnp.bfloat16)
            return carry
        lax.fori_loop(0, T // step, body, 0)

    def wait_bytes(ref, sem):
        pltpu.make_async_copy(ref, ref, sem).wait()

    wait_bytes(raw.at[:, pl.ds(0, T)], raw_sem.at[0])
    activate(0)
    wait_bytes(raw.at[:, pl.ds(T, T)], raw_sem.at[2])
    activate(1)

    def arrive(g):
        for a, dst in enumerate((tok_v, grad_v)):
            wait_bytes(dst.at[g, :, pl.ds(0, T)], load_sem.at[g, a])
            wait_bytes(dst.at[g, :, pl.ds(T, T)], swap_sem.at[g, a])

    def compute_block(g, u):
        feats, grads = tok_v[g, u], grad_v[g, u]
        for cls, (lo, hi) in enumerate(p.spans):
            pos = p.position(cls, u)
            for a, b in p.pieces(lo, hi, 2 * p.hidden):
                value = lax.dot_general(
                    feats if a < 2 * p.hidden else grads, hid[:, a:b],
                    (((0,), (0,)), ((), ())), preferred_element_type=jnp.float32,
                ).astype(jnp.bfloat16)
                for h in range(p.group):
                    m = g if p.group == 1 else g * p.group + flip(b_me % p.group, h)
                    terms[cls][m, pos, :, a - lo:b - lo] = value[h * R:(h + 1) * R]

    def compute(g):
        arrive(g)

        def body(u, carry):
            compute_block(g, u)
            return carry
        lax.fori_loop(0, C, body, 0)

    step = min(R, 32)

    def gather(cls, m, first, count, extra):
        def body(i, carry):
            blk, at = first + i // (R // step), pl.ds(pl.multiple_of((i % (R // step)) * step, step), step)
            value = terms[cls][m, blk, at, :].astype(jnp.float32)
            for ref, slot in extra:
                value = value + ref[slot, blk, at, :].astype(jnp.float32)
            terms[cls][m, blk, at, :] = value.astype(jnp.bfloat16)
            return carry
        if extra:
            lax.fori_loop(0, count * (R // step), body, 0)

    def finish(cls, extra):
        lo, hi = p.spans[cls]
        def body(i, carry):
            at = pl.ds(pl.multiple_of(i * step, step), step)
            for a, b in p.pieces(lo, hi, p.hidden):
                value = terms[cls][0, 0, at, a - lo:b - lo].astype(jnp.float32)
                for ref, slot in extra:
                    value = value + ref[slot, 0, at, a - lo:b - lo].astype(jnp.float32)
                base = (a // p.hidden) * p.hidden
                outs[a // p.hidden][at, a - base:b - base] = value
            return carry
        lax.fori_loop(0, R // step, body, 0)

    def seq_slot(cls, m):
        return 0 if p.batch_first[cls] else m

    def halves(stage):
        return 2 if C >> (stage + 1) > 1 else 1

    def seq_copy(cls, m, stage, part):
        count = C >> (stage + 1)
        size = count // halves(stage)
        first = count - size if part == 0 else 0
        slot = seq_slot(cls, m)
        return pltpu.make_async_remote_copy(
            src_ref=terms[cls].at[m, pl.ds(count + first, size)],
            dst_ref=seq_in[cls][stage].at[slot, pl.ds(first, size)],
            send_sem=seq_send.at[cls, 2 * stage + part, slot],
            recv_sem=seq_recv.at[cls, 2 * stage + part, slot],
            device_id=seq_peer[p.seq_bit(cls, stage)],
            device_id_type=MESH,
        )

    def batch_copy(cls, m):
        stage = low_bit(m)
        slot = m >> (stage + 1)
        count = C if p.batch_first[cls] else 1
        return pltpu.make_async_remote_copy(
            src_ref=terms[cls].at[m, pl.ds(0, count)],
            dst_ref=batch_in[cls][stage].at[slot],
            send_sem=batch_send.at[cls, stage, slot],
            recv_sem=batch_recv.at[cls, stage, slot],
            device_id=batch_peer[stage],
            device_id_type=MESH,
        )

    def start(copy):
        copy.start()
        sends.append(copy)

    def from_seq(cls, m, stages):
        return [(seq_in[cls][j], seq_slot(cls, m)) for j in range(stages)]

    def from_batch(cls, m):
        count = bb if m == 0 else low_bit(m)
        return [(batch_in[cls][j], m >> (j + 1)) for j in range(count)]

    def wait_batch(cls, m):
        count = bb if m == 0 else low_bit(m)
        for j in range(count):
            batch_copy(cls, m + (1 << j)).wait_recv()

    def wait_seq(cls, m, stage):
        if stage >= 0:
            seq_copy(cls, m, stage, 0).wait_recv()
        if stage >= 1:
            seq_copy(cls, m, stage - 1, 1).wait_recv()

    def seq_stage(cls, m, stage, base, parts=(0, 1)):
        wait_seq(cls, m, stage - 1)
        count = C >> (stage + 1)
        gather(cls, m, count, count, base + from_seq(cls, m, stage))
        for part in parts[:halves(stage)]:
            start(seq_copy(cls, m, stage, part))

    def batch_last(cls, m):
        wait_seq(cls, m, sb - 1)
        wait_batch(cls, m)
        extra = from_seq(cls, m, sb) + from_batch(cls, m)
        if m == 0:
            finish(cls, extra)
        else:
            gather(cls, m, 0, 1, extra)
            start(batch_copy(cls, m))

    def batch_early(cls, m):
        wait_batch(cls, m)
        if m:
            gather(cls, m, 0, C, from_batch(cls, m))
            start(batch_copy(cls, m))
        else:
            seq_stage(cls, 0, 0, from_batch(cls, 0))

    plain = [c for c in range(n_cls) if not p.batch_first[c]]
    early = [c for c in range(n_cls) if p.batch_first[c]]
    order = list(range(NB - 1, -1, -1))
    done = set()

    def need(i):
        if i < NB and order[i] // p.group not in done:
            done.add(order[i] // p.group)
            compute(order[i] // p.group)

    def first_round():
        g = groups[0]
        done.add(g)
        arrive(g)
        upper = [u for u in range(C) if any(p.position(c, u) >= C - C // 4 for c in plain)] if p.group == 1 else []
        for u in upper:
            compute_block(g, u)
        split = bool(upper) and halves(0) == 2
        if split:
            for cls in plain:
                start(seq_copy(cls, order[0], 0, 0))
        rest = [u for u in range(C) if u not in upper]
        if rest == list(range(len(rest))):
            def body(u, carry):
                compute_block(g, u)
                return carry
            lax.fori_loop(0, len(rest), body, 0)
        else:
            for u in rest:
                compute_block(g, u)
        for cls in plain:
            for part in range(1 if split else 0, halves(0)):
                start(seq_copy(cls, order[0], 0, part))
        if order[0] % 2:
            for cls in early:
                batch_early(cls, order[0])

    first_round()
    for i in range(1, NB + 1):
        before = order[i - 1]
        need(i)
        if i == 1:
            need(2)
        for stage in range(1, sb):
            for cls in plain:
                seq_stage(cls, before, stage, [])
        if i < NB:
            for cls in plain:
                seq_stage(cls, order[i], 0, [])
        if i + 1 < NB:
            need(i + 1)
        for cls in early:
            if i + 1 < NB and order[i + 1] % 2:
                batch_early(cls, order[i + 1])
            if i < NB and order[i] and order[i] % 2 == 0:
                batch_early(cls, order[i])
        if i == NB:
            for cls in early:
                batch_early(cls, 0)
        for cls in plain:
            batch_last(cls, before)
    for stage in range(1, sb):
        for cls in early:
            seq_stage(cls, 0, stage, from_batch(cls, 0))
    for cls in early:
        wait_seq(cls, 0, sb - 1)
        finish(cls, from_batch(cls, 0) + from_seq(cls, 0, sb))

    for copy in sends:
        copy.wait_send()
    wait_bytes(raw.at[:, pl.ds(T, T)], raw_sem.at[1])
    for g in groups:
        for a, dst in enumerate((tok_v, grad_v)):
            wait_bytes(dst.at[g, :, pl.ds(T, T)], swap_out.at[g, a])


X, Y, Z0, Z1 = range(4)


class Flow:
    def __init__(self, source, order, rows, cols, out, out_col):
        self.source, self.order, self.rows, self.cols = source, order, rows, cols
        self.out, self.out_col = out, out_col
        self.n = len(order)
        self.shape = (1 << self.n, rows[1] - rows[0], cols[1] - cols[0])

    def dense(self, block):
        return sum(((block >> b) & 1) << (self.n - 1 - i) for i, b in enumerate(self.order))

    def block(self, d):
        return sum(((d >> (self.n - 1 - i)) & 1) << b for i, b in enumerate(self.order))

    def stage(self, d):
        return self.n - d.bit_length()

    def incoming(self, d):
        return [d + (1 << (self.n - 1 - i)) for i in range(self.stage(d))]


class Exchange:
    def __init__(self, n_batch, n_seq, tok, width, hidden):
        self.n_batch, self.n_seq, self.tok, self.width, self.hidden = n_batch, n_seq, tok, width, hidden
        self.rows = R = width // (n_batch * n_seq)
        unit, half = hidden // 6, R // 2
        full = (0, R)
        batch_first, y_first, x_first = (Z0, Z1, X, Y), (Y, X, Z0, Z1), (X, Y, Z0, Z1)
        def down(order, rows, a, b):
            return Flow("down", order, rows, (a * unit, b * unit), 2, 0)
        self.flows = [
            Flow("up", (Y, Z0, Z1), full, (0, hidden), 0, 0),
            Flow("up", (Y, Z0, Z1), full, (hidden, 2 * hidden), 1, hidden),
            down(batch_first, full, 0, 2),
            down(batch_first, (0, half), 2, 3),
            down(x_first, (half, R), 2, 3),
            down(y_first, full, 3, 6),
        ]

    @staticmethod
    def fits(n_batch, n_seq, tok, width, hidden):
        return n_batch == 4 and n_seq == 8 and hidden % (6 * LANES) == 0 and width % (n_batch * n_seq * LANES) == 0

    def tasks(self):
        out = [("tok", k, m) for k in (1, 0) for m in (3, 1, 2, 0)]
        out += [("forward",)]
        out += [("down", u, m) for u in range(4) for m in range(4)]
        out += [("up", k, m) for k in range(2) for m in range(4)]
        out += [("advance", c, d) for c, f in enumerate(self.flows) for d in range(1 << f.n)]
        return out


ORDER = (
    18, 107, 58, 22, 21, 60, 9, 14, 20, 109, 16, 10, 15, 63, 19, 24,
    17, 12, 11, 23, 112, 62, 13, 64, 108, 61, 111, 55, 54, 110, 56, 104,
    105, 59, 4, 57, 106, 8, 53, 32, 40, 102, 100, 79, 2, 78, 73, 75,
    80, 28, 48, 74, 77, 76, 1, 98, 70, 71, 36, 31, 38, 6, 44, 46,
    30, 94, 5, 72, 27, 39, 34, 96, 103, 92, 52, 26, 95, 88, 42, 3,
    47, 51, 35, 87, 50, 90, 93, 101, 86, 29, 37, 89, 84, 91, 99, 7,
    49, 43, 45, 68, 67, 97, 82, 85, 83, 69, 25, 66, 33, 41, 81, 65,
)


def exchange_kernel(plan, tokens, out_grad, gate_pre, up_pre, hidden_grad, out_gate, out_up, out_down, *scratch):
    p = plan
    T, R, F, NB = p.tok, p.rows, p.hidden, p.n_batch
    n_flows = len(p.flows)
    scratch = list(scratch)
    raw, hid, cot, tok_v, grad_v = (scratch.pop(0) for _ in range(5))
    own = [scratch.pop(0) for _ in range(n_flows)]
    got = [scratch.pop(0) for _ in range(n_flows)]
    raw_sem, cot_sem, load_g, swap_g, sent_g, load_t, swap_t, sent_t, send_x, recv_x, flow_send, flow_recv = scratch
    outs = (out_gate, out_up, out_down)

    b_me, s_me = lax.axis_index("batch"), lax.axis_index("seq")
    core, chip = s_me % 2, s_me // 2

    def device(block, other=0):
        return (flip(b_me, block >> 2), flip(s_me, 2 * (block & 3) + other))

    def columns(block, other=0):
        b, s = device(block, other)
        return pl.ds(pl.multiple_of((s * NB + b) * R, R), R)

    twin, across, crossed = device(0, 1), device(1 << X), device(1 << X, 1)
    peer = [device(1 << bit) for bit in range(4)]
    sends = []

    def remote(src, dst, send_sem, recv_sem, to):
        return pltpu.make_async_remote_copy(
            src_ref=src, dst_ref=dst, send_sem=send_sem, recv_sem=recv_sem, device_id=to, device_id_type=MESH
        )

    def start(copy):
        copy.start()
        sends.append(copy)

    def raw_copies():
        return [pltpu.make_async_copy(ref, raw.at[i, pl.ds(0, T)], raw_sem.at[0, i])
                for i, ref in enumerate((gate_pre, up_pre, hidden_grad))]

    def raw_swaps():
        return [remote(ref, raw.at[i, pl.ds(T, T)], raw_sem.at[1, i], raw_sem.at[2, i], twin)
                for i, ref in enumerate((gate_pre, up_pre, hidden_grad))]

    def grad_copy(u, m):
        return pltpu.make_async_copy(
            out_grad.at[:, columns(u + 4 * m)], grad_v.at[u, m, pl.ds(0, T)], load_g.at[u, m])

    def grad_swap(u, m):
        return remote(out_grad.at[:, columns(u + 4 * m, 1)], grad_v.at[u, m, pl.ds(T, T)],
                      sent_g.at[u, m], swap_g.at[u, m], twin)

    def tok_copy(k, m):
        return pltpu.make_async_copy(
            tokens.at[:, columns(2 * k + 4 * m)], tok_v.at[k, m, pl.ds(0, T)], load_t.at[k, m])

    def tok_swap(k, m):
        return remote(tokens.at[:, columns(2 * k + 4 * m, 1)], tok_v.at[k, m, pl.ds(T, T)],
                      sent_t.at[k, m], swap_t.at[k, m], twin)

    def tok_sends(k, m):
        return [remote(tokens.at[:, columns(1 + 2 * k + 4 * m, c)], tok_v.at[k, m, pl.ds((2 + c) * T, T)],
                       send_x.at[k, m, c], recv_x.at[k, m, c], to) for c, to in enumerate((across, crossed))]

    def cot_send():
        return remote(cot.at[pl.ds(0, T)], cot.at[pl.ds(2 * T, T)], cot_sem.at[0], cot_sem.at[1], across)

    def cot_forward():
        return remote(cot.at[pl.ds(2 * T, T)], cot.at[pl.ds(3 * T, T)], cot_sem.at[2], cot_sem.at[3], twin)

    def flow_copy(c, d):
        f = p.flows[c]
        return remote(own[c].at[d], got[c].at[d], flow_send.at[c, d], flow_recv.at[c, d], peer[f.order[f.stage(d)]])

    def activate(side):
        step = 32
        def body(i, carry):
            at = pl.ds(pl.multiple_of(side * T + i * step, step), step)
            gate_val = raw[0, at, :].astype(jnp.float32)
            up_val = raw[1, at, :].astype(jnp.float32)
            grad_val = raw[2, at, :].astype(jnp.float32)
            sig = jax.nn.sigmoid(gate_val)
            act = gate_val * sig
            cot[at, 0:F] = (grad_val * up_val * sig * (1.0 + gate_val * (1.0 - sig))).astype(jnp.bfloat16)
            cot[at, F:2 * F] = (grad_val * act).astype(jnp.bfloat16)
            hid[at, :] = (act * up_val).astype(jnp.bfloat16)
            return carry
        lax.fori_loop(0, T // step, body, 0)

    dot = functools.partial(
        lax.dot_general, dimension_numbers=(((0,), (0,)), ((), ())), preferred_element_type=jnp.float32)

    def keep(source, block, value):
        for c, f in enumerate(p.flows):
            if f.source == source:
                own[c][f.dense(block)] = value[f.rows[0]:f.rows[1], f.cols[0]:f.cols[1]].astype(jnp.bfloat16)

    def down(u, m):
        grad_copy(u, m).wait()
        grad_swap(u, m).wait_recv()
        keep("down", u + 4 * m, dot(grad_v[u, m], hid[...]))

    cot_left = [True]

    def up(k, m):
        if cot_left:
            cot_left.pop()
            cot_forward().wait_recv()
        tok_copy(k, m).wait()
        tok_swap(k, m).wait_recv()
        for copy in tok_sends(k, m):
            copy.wait_recv()
        keep("up", 2 * k + 4 * m, dot(tok_v[k, m], cot[...]))

    def tok(k, m):
        for copy in tok_sends(k, m):
            start(copy)

    def forward():
        cot_send().wait_recv()
        start(cot_forward())

    def advance(c, d):
        f = p.flows[c]
        entries = f.incoming(d)
        for e in entries:
            flow_copy(c, e).wait_recv()
        rows = f.shape[1]
        step = 32

        def body(i, carry):
            at = pl.ds(pl.multiple_of(i * step, step), step)
            value = own[c][d, at, :].astype(jnp.float32)
            for e in entries:
                value = value + got[c][e, at, :].astype(jnp.float32)
            if d:
                own[c][d, at, :] = value.astype(jnp.bfloat16)
            else:
                to = pl.ds(pl.multiple_of(f.rows[0] + i * step, step), step)
                outs[f.out][to, f.cols[0] - f.out_col:f.cols[1] - f.out_col] = value
            return carry
        if entries:
            lax.fori_loop(0, rows // step, body, 0)
        if d:
            start(flow_copy(c, d))

    tasks = p.tasks()
    order = [tasks[i] for i in ORDER]
    downs = [t[1:] for t in order if t[0] == "down"]
    ups = [t[1:] for t in order if t[0] == "up"]

    for copy in raw_copies():
        copy.start()
    for u, m in downs:
        grad_copy(u, m).start()
    for k, m in ups:
        tok_copy(k, m).start()

    barrier = pltpu.get_barrier_semaphore()
    peers = [twin, crossed] + peer
    for to in peers:
        pl.semaphore_signal(barrier, inc=1, device_id=to, device_id_type=MESH)
    pl.semaphore_wait(barrier, len(peers))

    for copy in raw_swaps():
        start(copy)
    tok(1, 3)
    for u, m in downs:
        start(grad_swap(u, m))
    for copy in raw_copies():
        copy.wait()
    activate(0)
    start(cot_send())
    for k, m in ups:
        start(tok_swap(k, m))
    for copy in raw_swaps():
        copy.wait_recv()
    activate(1)

    run = {"tok": tok, "forward": forward, "down": down, "up": up, "advance": advance}
    for task in order:
        run[task[0]](*task[1:])

    for copy in sends:
        copy.wait_send()


def exchange_on_device(p, *args):
    T, R, F, bf16 = p.tok, p.rows, p.hidden, jnp.bfloat16
    scratch = [
        pltpu.VMEM((3, 2 * T, F), bf16),
        pltpu.VMEM((2 * T, F), bf16),
        pltpu.VMEM((4 * T, 2 * F), bf16),
        pltpu.VMEM((2, 4, 4 * T, R), bf16),
        pltpu.VMEM((4, 4, 2 * T, R), bf16),
    ]
    scratch += [pltpu.VMEM(f.shape, bf16) for f in p.flows] * 2
    dma, n_flows = pltpu.SemaphoreType.DMA, len(p.flows)
    scratch += [dma((3, 3)), dma((4,))] + [dma((4, 4))] * 3 + [dma((2, 4))] * 3
    scratch += [dma((2, 4, 2))] * 2 + [dma((n_flows, 16))] * 2
    out = jax.ShapeDtypeStruct((R, F), jnp.float32)
    return pl.pallas_call(
        functools.partial(exchange_kernel, p),
        out_shape=(out, out, out),
        in_specs=[pl.BlockSpec(memory_space=pltpu.HBM)] * 5,
        out_specs=[pl.BlockSpec(memory_space=pltpu.VMEM)] * 3,
        scratch_shapes=scratch,
        compiler_params=pltpu.CompilerParams(
            collective_id=0, has_side_effects=True, vmem_limit_bytes=67043328
        ),
    )(*args)


def on_device(n_batch, n_seq, tokens, out_grad, gate_pre, up_pre, hidden_grad):
    tok, width = tokens.shape
    hidden = gate_pre.shape[1]
    sizes = (n_batch, n_seq, tok, width, hidden)
    if Exchange.fits(*sizes):
        return exchange_on_device(
            Exchange(*sizes), tokens, out_grad, gate_pre, up_pre, hidden_grad
        )
    p = Plan(*sizes)
    C, R, bf16 = p.chips, p.rows, jnp.bfloat16
    scratch = [
        pltpu.VMEM((3, 2 * tok, hidden), bf16),
        pltpu.VMEM((2 * tok, 3 * hidden), bf16),
        pltpu.VMEM((p.n_groups, C, 2 * tok, p.block), bf16),
        pltpu.VMEM((p.n_groups, C, 2 * tok, p.block), bf16),
    ]
    sizes = [hi - lo for lo, hi in p.spans]
    scratch += [pltpu.VMEM((n_batch, C, R, size), bf16) for size in sizes]
    for cls, size in enumerate(sizes):
        slots = 1 if p.batch_first[cls] else n_batch
        scratch += [pltpu.VMEM((slots, C >> (j + 1), R, size), bf16) for j in range(p.seq_bits)]
    for cls, size in enumerate(sizes):
        blocks = C if p.batch_first[cls] else 1
        scratch += [pltpu.VMEM((n_batch >> (j + 1), blocks, R, size), bf16) for j in range(p.batch_bits)]
    n_cls = len(sizes)
    dma = pltpu.SemaphoreType.DMA
    scratch += [
        dma((3,)),
        dma((p.n_groups, 2)), dma((p.n_groups, 2)), dma((p.n_groups, 2)),
        dma((n_cls, 2 * p.seq_bits, n_batch)), dma((n_cls, 2 * p.seq_bits, n_batch)),
        dma((n_cls, p.batch_bits, n_batch // 2)), dma((n_cls, p.batch_bits, n_batch // 2)),
    ]
    out = jax.ShapeDtypeStruct((R, hidden), jnp.float32)
    return pl.pallas_call(
        functools.partial(kernel, p),
        out_shape=(out, out, out),
        in_specs=[pl.BlockSpec(memory_space=pltpu.HBM)] * 5,
        out_specs=[pl.BlockSpec(memory_space=pltpu.VMEM)] * 3,
        scratch_shapes=scratch,
        compiler_params=pltpu.CompilerParams(
            collective_id=0, has_side_effects=True, vmem_limit_bytes=67043328
        ),
    )(tokens, out_grad, gate_pre, up_pre, hidden_grad)


def solution(mesh):
    rows = P(("batch", "seq"), None)
    outs = P(("seq", "batch"), None)
    body = functools.partial(on_device, mesh.shape["batch"], mesh.shape["seq"])
    return jax.shard_map(
        body, mesh=mesh, in_specs=(rows,) * 5, out_specs=(outs,) * 3, check_vma=False
    )
```

```python
import functools
import math

import jax
import jax.numpy as jnp
from jax import lax
from jax.experimental import pallas as pl
from jax.experimental.pallas import tpu as pltpu
from jax.sharding import PartitionSpec as P

MESH = pl.DeviceIdType.MESH
LANES = 128


def bit_count(n):
    return n.bit_length() - 1


def flip(value, mask):
    out, bit = value, 1
    while bit <= mask:
        if mask & bit:
            out = out + bit * (1 - 2 * ((value // bit) % 2))
        bit *= 2
    return out


class Plan:
    def __init__(self, n_batch, n_seq, tok, width, hidden):
        self.n_batch, self.n_seq, self.tok, self.width, self.hidden = n_batch, n_seq, tok, width, hidden
        self.chips = n_seq // 2
        self.seq_bits, self.batch_bits = bit_count(self.chips), bit_count(n_batch)
        self.rows = width // (n_batch * n_seq)
        self.group = max(1, LANES // self.rows)
        self.block = self.group * self.rows
        self.n_groups = n_batch // self.group
        total = 3 * hidden
        units = total // LANES
        late = max(2, units // 6)
        early = (units - late) // 2
        cuts = [0, early, units - late, units - late // 2, units]
        self.spans = [(a * LANES, b * LANES) for a, b in zip(cuts[:-1], cuts[1:])]
        self.ascending = [True, False, True, False]
        self.batch_first = [False, False, True, True]

    def seq_bit(self, cls, stage):
        return stage if self.ascending[cls] else self.seq_bits - 1 - stage

    def position(self, cls, u):
        if not self.ascending[cls]:
            return u
        return sum(((u // (1 << i)) % 2) * (1 << (self.seq_bits - 1 - i)) for i in range(self.seq_bits))

    def pieces(self, lo, hi, step):
        out = []
        while lo < hi:
            end = min(hi, (lo // step + 1) * step)
            out.append((lo, end))
            lo = end
        return out


def low_bit(m):
    return (m & -m).bit_length() - 1


def kernel(plan, tokens, out_grad, gate_pre, up_pre, hidden_grad, out_gate, out_up, out_down, *scratch):
    p = plan
    T, R, M, C, NB = p.tok, p.rows, p.block, p.chips, p.n_batch
    n_cls, sb, bb = len(p.spans), p.seq_bits, p.batch_bits
    scratch = list(scratch)
    raw, hid, tok_v, grad_v = (scratch.pop(0) for _ in range(4))
    terms = [scratch.pop(0) for _ in range(n_cls)]
    seq_in = [[scratch.pop(0) for _ in range(sb)] for _ in range(n_cls)]
    batch_in = [[scratch.pop(0) for _ in range(bb)] for _ in range(n_cls)]
    raw_sem, load_sem, swap_sem, swap_out, seq_send, seq_recv, batch_send, batch_recv = scratch
    outs = (out_gate, out_up, out_down)

    b_me, s_me = lax.axis_index("batch"), lax.axis_index("seq")
    core, chip = s_me % 2, s_me // 2
    twin = (b_me, s_me + 1 - 2 * core)
    seq_peer = [(b_me, flip(s_me, 2 << i)) for i in range(sb)]
    batch_peer = [(flip(b_me, 1 << i), s_me) for i in range(bb)]

    pre = (gate_pre, up_pre, hidden_grad)
    for i, ref in enumerate(pre):
        pltpu.make_async_copy(ref, raw.at[i, pl.ds(0, T)], raw_sem.at[0]).start()

    def column(g, u, side):
        k = flip(chip, u)
        first = flip(b_me // p.group, g) * p.group
        return pl.multiple_of(((k * 2 + side) * NB + first) * R, M)

    sends = []
    groups = list(range(p.n_groups - 1, -1, -1))

    def load(g):
        for a, (src, dst) in enumerate(((tokens, tok_v), (out_grad, grad_v))):
            for u in range(C):
                pltpu.make_async_copy(
                    src.at[:, pl.ds(column(g, u, core), M)], dst.at[g, u, pl.ds(0, T)], load_sem.at[g, a]
                ).start()

    def swap(g):
        for a, (src, dst) in enumerate(((tokens, tok_v), (out_grad, grad_v))):
            for u in range(C):
                pltpu.make_async_remote_copy(
                    src_ref=src.at[:, pl.ds(column(g, u, 1 - core), M)],
                    dst_ref=dst.at[g, u, pl.ds(T, T)],
                    send_sem=swap_out.at[g, a],
                    recv_sem=swap_sem.at[g, a],
                    device_id=twin,
                    device_id_type=MESH,
                ).start()

    for g in groups:
        load(g)

    barrier = pltpu.get_barrier_semaphore()
    peers = [twin] + seq_peer + batch_peer
    for peer in peers:
        pl.semaphore_signal(barrier, inc=1, device_id=peer, device_id_type=MESH)
    pl.semaphore_wait(barrier, len(peers))

    for i, ref in enumerate(pre):
        pltpu.make_async_remote_copy(
            src_ref=ref, dst_ref=raw.at[i, pl.ds(T, T)], send_sem=raw_sem.at[1], recv_sem=raw_sem.at[2],
            device_id=twin, device_id_type=MESH,
        ).start()
    for g in groups:
        swap(g)

    def activate(side):
        step = 32
        def body(i, carry):
            at = pl.ds(pl.multiple_of(side * T + i * step, step), step)
            gate_val = raw[0, at, :].astype(jnp.float32)
            up_val = raw[1, at, :].astype(jnp.float32)
            grad_val = raw[2, at, :].astype(jnp.float32)
            sig = jax.nn.sigmoid(gate_val)
            act = gate_val * sig
            F = p.hidden
            hid[at, 0:F] = (grad_val * up_val * sig * (1.0 + gate_val * (1.0 - sig))).astype(jnp.bfloat16)
            hid[at, F:2 * F] = (grad_val * act).astype(jnp.bfloat16)
            hid[at, 2 * F:3 * F] = (act * up_val).astype(jnp.bfloat16)
            return carry
        lax.fori_loop(0, T // step, body, 0)

    def wait_bytes(ref, sem):
        pltpu.make_async_copy(ref, ref, sem).wait()

    wait_bytes(raw.at[:, pl.ds(0, T)], raw_sem.at[0])
    activate(0)
    wait_bytes(raw.at[:, pl.ds(T, T)], raw_sem.at[2])
    activate(1)

    def arrive(g):
        for a, dst in enumerate((tok_v, grad_v)):
            wait_bytes(dst.at[g, :, pl.ds(0, T)], load_sem.at[g, a])
            wait_bytes(dst.at[g, :, pl.ds(T, T)], swap_sem.at[g, a])

    def compute_block(g, u):
        feats, grads = tok_v[g, u], grad_v[g, u]
        for cls, (lo, hi) in enumerate(p.spans):
            pos = p.position(cls, u)
            for a, b in p.pieces(lo, hi, 2 * p.hidden):
                value = lax.dot_general(
                    feats if a < 2 * p.hidden else grads, hid[:, a:b],
                    (((0,), (0,)), ((), ())), preferred_element_type=jnp.float32,
                ).astype(jnp.bfloat16)
                for h in range(p.group):
                    m = g if p.group == 1 else g * p.group + flip(b_me % p.group, h)
                    terms[cls][m, pos, :, a - lo:b - lo] = value[h * R:(h + 1) * R]

    def compute(g):
        arrive(g)

        def body(u, carry):
            compute_block(g, u)
            return carry
        lax.fori_loop(0, C, body, 0)

    step = min(R, 32)

    def gather(cls, m, first, count, extra):
        def body(i, carry):
            blk, at = first + i // (R // step), pl.ds(pl.multiple_of((i % (R // step)) * step, step), step)
            value = terms[cls][m, blk, at, :].astype(jnp.float32)
            for ref, slot in extra:
                value = value + ref[slot, blk, at, :].astype(jnp.float32)
            terms[cls][m, blk, at, :] = value.astype(jnp.bfloat16)
            return carry
        if extra:
            lax.fori_loop(0, count * (R // step), body, 0)

    def finish(cls, extra):
        lo, hi = p.spans[cls]
        def body(i, carry):
            at = pl.ds(pl.multiple_of(i * step, step), step)
            for a, b in p.pieces(lo, hi, p.hidden):
                value = terms[cls][0, 0, at, a - lo:b - lo].astype(jnp.float32)
                for ref, slot in extra:
                    value = value + ref[slot, 0, at, a - lo:b - lo].astype(jnp.float32)
                base = (a // p.hidden) * p.hidden
                outs[a // p.hidden][at, a - base:b - base] = value
            return carry
        lax.fori_loop(0, R // step, body, 0)

    def seq_slot(cls, m):
        return 0 if p.batch_first[cls] else m

    def halves(stage):
        return 2 if C >> (stage + 1) > 1 else 1

    def seq_copy(cls, m, stage, part):
        count = C >> (stage + 1)
        size = count // halves(stage)
        first = count - size if part == 0 else 0
        slot = seq_slot(cls, m)
        return pltpu.make_async_remote_copy(
            src_ref=terms[cls].at[m, pl.ds(count + first, size)],
            dst_ref=seq_in[cls][stage].at[slot, pl.ds(first, size)],
            send_sem=seq_send.at[cls, 2 * stage + part, slot],
            recv_sem=seq_recv.at[cls, 2 * stage + part, slot],
            device_id=seq_peer[p.seq_bit(cls, stage)],
            device_id_type=MESH,
        )

    def batch_copy(cls, m):
        stage = low_bit(m)
        slot = m >> (stage + 1)
        count = C if p.batch_first[cls] else 1
        return pltpu.make_async_remote_copy(
            src_ref=terms[cls].at[m, pl.ds(0, count)],
            dst_ref=batch_in[cls][stage].at[slot],
            send_sem=batch_send.at[cls, stage, slot],
            recv_sem=batch_recv.at[cls, stage, slot],
            device_id=batch_peer[stage],
            device_id_type=MESH,
        )

    def start(copy):
        copy.start()
        sends.append(copy)

    def from_seq(cls, m, stages):
        return [(seq_in[cls][j], seq_slot(cls, m)) for j in range(stages)]

    def from_batch(cls, m):
        count = bb if m == 0 else low_bit(m)
        return [(batch_in[cls][j], m >> (j + 1)) for j in range(count)]

    def wait_batch(cls, m):
        count = bb if m == 0 else low_bit(m)
        for j in range(count):
            batch_copy(cls, m + (1 << j)).wait_recv()

    def wait_seq(cls, m, stage):
        if stage >= 0:
            seq_copy(cls, m, stage, 0).wait_recv()
        if stage >= 1:
            seq_copy(cls, m, stage - 1, 1).wait_recv()

    def seq_stage(cls, m, stage, base, parts=(0, 1)):
        wait_seq(cls, m, stage - 1)
        count = C >> (stage + 1)
        gather(cls, m, count, count, base + from_seq(cls, m, stage))
        for part in parts[:halves(stage)]:
            start(seq_copy(cls, m, stage, part))

    def batch_last(cls, m):
        wait_seq(cls, m, sb - 1)
        wait_batch(cls, m)
        extra = from_seq(cls, m, sb) + from_batch(cls, m)
        if m == 0:
            finish(cls, extra)
        else:
            gather(cls, m, 0, 1, extra)
            start(batch_copy(cls, m))

    def batch_early(cls, m):
        wait_batch(cls, m)
        if m:
            gather(cls, m, 0, C, from_batch(cls, m))
            start(batch_copy(cls, m))
        else:
            seq_stage(cls, 0, 0, from_batch(cls, 0))

    plain = [c for c in range(n_cls) if not p.batch_first[c]]
    early = [c for c in range(n_cls) if p.batch_first[c]]
    order = list(range(NB - 1, -1, -1))
    done = set()

    def need(i):
        if i < NB and order[i] // p.group not in done:
            done.add(order[i] // p.group)
            compute(order[i] // p.group)

    def first_round():
        g = groups[0]
        done.add(g)
        arrive(g)
        upper = [u for u in range(C) if any(p.position(c, u) >= C - C // 4 for c in plain)] if p.group == 1 else []
        for u in upper:
            compute_block(g, u)
        split = bool(upper) and halves(0) == 2
        if split:
            for cls in plain:
                start(seq_copy(cls, order[0], 0, 0))
        rest = [u for u in range(C) if u not in upper]
        if rest == list(range(len(rest))):
            def body(u, carry):
                compute_block(g, u)
                return carry
            lax.fori_loop(0, len(rest), body, 0)
        else:
            for u in rest:
                compute_block(g, u)
        for cls in plain:
            for part in range(1 if split else 0, halves(0)):
                start(seq_copy(cls, order[0], 0, part))
        if order[0] % 2:
            for cls in early:
                batch_early(cls, order[0])

    first_round()
    for i in range(1, NB + 1):
        before = order[i - 1]
        need(i)
        if i == 1:
            need(2)
        for stage in range(1, sb):
            for cls in plain:
                seq_stage(cls, before, stage, [])
        if i < NB:
            for cls in plain:
                seq_stage(cls, order[i], 0, [])
        if i + 1 < NB:
            need(i + 1)
        for cls in early:
            if i + 1 < NB and order[i + 1] % 2:
                batch_early(cls, order[i + 1])
            if i < NB and order[i] and order[i] % 2 == 0:
                batch_early(cls, order[i])
        if i == NB:
            for cls in early:
                batch_early(cls, 0)
        for cls in plain:
            batch_last(cls, before)
    for stage in range(1, sb):
        for cls in early:
            seq_stage(cls, 0, stage, from_batch(cls, 0))
    for cls in early:
        wait_seq(cls, 0, sb - 1)
        finish(cls, from_batch(cls, 0) + from_seq(cls, 0, sb))

    for copy in sends:
        copy.wait_send()
    wait_bytes(raw.at[:, pl.ds(T, T)], raw_sem.at[1])
    for g in groups:
        for a, dst in enumerate((tok_v, grad_v)):
            wait_bytes(dst.at[g, :, pl.ds(T, T)], swap_out.at[g, a])


X, Y, Z0, Z1 = range(4)


class Flow:
    def __init__(self, source, order, rows, cols, out, out_col):
        self.source, self.order, self.rows, self.cols = source, order, rows, cols
        self.out, self.out_col = out, out_col
        self.n = len(order)
        self.shape = (1 << self.n, rows[1] - rows[0], cols[1] - cols[0])

    def dense(self, block):
        return sum(((block >> b) & 1) << (self.n - 1 - i) for i, b in enumerate(self.order))

    def block(self, d):
        return sum(((d >> (self.n - 1 - i)) & 1) << b for i, b in enumerate(self.order))

    def stage(self, d):
        return self.n - d.bit_length()

    def incoming(self, d):
        return [d + (1 << (self.n - 1 - i)) for i in range(self.stage(d))]


class Exchange:
    def __init__(self, n_batch, n_seq, tok, width, hidden):
        self.n_batch, self.n_seq, self.tok, self.width, self.hidden = n_batch, n_seq, tok, width, hidden
        self.rows = R = width // (n_batch * n_seq)
        unit, half = hidden // 6, R // 2
        full = (0, R)
        batch_first, y_first, x_first = (Z0, Z1, X, Y), (Y, X, Z0, Z1), (X, Y, Z0, Z1)
        def down(order, rows, a, b):
            return Flow("down", order, rows, (a * unit, b * unit), 2, 0)
        self.flows = [
            Flow("up", (Y, Z0, Z1), full, (0, hidden), 0, 0),
            Flow("up", (Y, Z0, Z1), full, (hidden, 2 * hidden), 1, hidden),
            down(batch_first, full, 0, 2),
            down(batch_first, (0, half), 2, 3),
            down(x_first, (half, R), 2, 3),
            down(y_first, full, 3, 6),
        ]

    @staticmethod
    def fits(n_batch, n_seq, tok, width, hidden):
        return n_batch == 4 and n_seq == 8 and hidden % (6 * LANES) == 0 and width % (n_batch * n_seq * LANES) == 0

    def tasks(self):
        out = [("tok", k, m) for k in (1, 0) for m in (3, 1, 2, 0)]
        out += [("forward",)]
        out += [("down", u, m) for u in range(4) for m in range(4)]
        out += [("up", k, m) for k in range(2) for m in range(4)]
        out += [("advance", c, d) for c, f in enumerate(self.flows) for d in range(1 << f.n)]
        return out


SPARE = 6 << 20
ORDER = (
    22, 111, 60, 14, 15, 59, 24, 23, 19, 112, 13, 10, 16, 79, 20, 78,
    12, 17, 57, 9, 21, 108, 11, 18, 74, 73, 80, 61, 71, 107, 70, 64,
    109, 72, 76, 62, 53, 106, 8, 56, 105, 104, 58, 54, 110, 4, 32, 48,
    75, 63, 2, 100, 40, 77, 28, 55, 1, 44, 69, 31, 6, 46, 36, 30,
    5, 47, 27, 42, 3, 38, 26, 94, 102, 43, 39, 7, 29, 34, 89, 86,
    96, 45, 92, 67, 90, 101, 25, 35, 103, 88, 37, 93, 98, 68, 91, 95,
    52, 41, 51, 84, 99, 85, 66, 87, 50, 82, 33, 65, 83, 97, 49, 81,
)


def exchange_kernel(plan, tokens, out_grad, gate_cot, up_cot, hidden, out_gate, out_up, out_down, *scratch):
    p = plan
    T, R, F, NB = p.tok, p.rows, p.hidden, p.n_batch
    n_flows = len(p.flows)
    scratch = list(scratch)
    hid, cot, tok_v, grad_v = (scratch.pop(0) for _ in range(4))
    own = [scratch.pop(0) for _ in range(n_flows)]
    got = [scratch.pop(0) for _ in range(n_flows)]
    cot_sem, grad_sem, tok_sem, swap_sent, flow_sent = (scratch.pop(0) for _ in range(5))
    flow_got = scratch
    outs = (out_gate, out_up, out_down)

    b_me, s_me = lax.axis_index("batch"), lax.axis_index("seq")
    core, chip = s_me % 2, s_me // 2

    def device(block, other=0):
        return (flip(b_me, block >> 2), flip(s_me, 2 * (block & 3) + other))

    def columns(block, other=0):
        b, s = device(block, other)
        return pl.ds(pl.multiple_of((s * NB + b) * R, R), R)

    twin, across, crossed = device(0, 1), device(1 << X), device(1 << X, 1)
    peer = [device(1 << bit) for bit in range(4)]

    def remote(src, dst, send_sem, recv_sem, to):
        return pltpu.make_async_remote_copy(
            src_ref=src, dst_ref=dst, send_sem=send_sem, recv_sem=recv_sem, device_id=to, device_id_type=MESH
        )

    def wait_bytes(ref, sem):
        pltpu.make_async_copy(ref, ref, sem).wait()

    def grad_copy(u, m):
        return pltpu.make_async_copy(
            out_grad.at[:, columns(u + 4 * m)], grad_v.at[u, m, pl.ds(0, T)], grad_sem.at[u, m])

    def grad_swap(u, m):
        return remote(out_grad.at[:, columns(u + 4 * m, 1)], grad_v.at[u, m, pl.ds(T, T)],
                      swap_sent.at[0], grad_sem.at[u, m], twin)

    def tok_copy(k, m):
        return pltpu.make_async_copy(
            tokens.at[:, columns(2 * k + 4 * m)], tok_v.at[k, m, pl.ds(0, T)], tok_sem.at[k, m])

    def tok_swap(k, m):
        return remote(tokens.at[:, columns(2 * k + 4 * m, 1)], tok_v.at[k, m, pl.ds(T, T)],
                      swap_sent.at[1], tok_sem.at[k, m], twin)

    def tok_send(k, m, c):
        return remote(tokens.at[:, columns(1 + 2 * k + 4 * m, c)], tok_v.at[k, m, pl.ds((2 + c) * T, T)],
                      swap_sent.at[2], tok_sem.at[k, m], crossed if c else across)

    def cot_slot(slot):
        return cot.at[pl.ds(slot * T, T)]

    def cot_send(slot, to):
        for i, ref in enumerate((gate_cot, up_cot)):
            remote(ref, cot.at[pl.ds(slot * T, T), pl.ds(i * F, F)], cot_sem.at[0], cot_sem.at[slot], to).start()

    def cot_forward():
        return remote(cot_slot(2), cot_slot(3), cot_sem.at[4], cot_sem.at[3], twin)

    def hid_swap():
        return remote(hidden, hid.at[pl.ds(T, T)], cot_sem.at[5], cot_sem.at[6], twin)

    def flow_copy(c, d):
        f = p.flows[c]
        to = d - (1 << (f.n - 1 - f.stage(d)))
        return remote(own[c].at[d], got[c].at[d], flow_sent.at[c], flow_got[c].at[to], peer[f.order[f.stage(d)]])

    dot = functools.partial(
        lax.dot_general, dimension_numbers=(((0,), (0,)), ((), ())), preferred_element_type=jnp.float32)

    def keep(source, block, value):
        for c, f in enumerate(p.flows):
            if f.source == source:
                own[c][f.dense(block)] = value[f.rows[0]:f.rows[1], f.cols[0]:f.cols[1]].astype(jnp.bfloat16)

    waits = {"hid", "cot"}

    def down(u, m):
        if "hid" in waits:
            waits.remove("hid")
            hid_swap().wait_recv()
        wait_bytes(grad_v.at[u, m], grad_sem.at[u, m])
        keep("down", u + 4 * m, dot(grad_v[u, m], hid[...]))

    def up(k, m):
        if "cot" in waits:
            waits.remove("cot")
            wait_bytes(cot_slot(1), cot_sem.at[1])
            cot_forward().wait_recv()
        wait_bytes(tok_v.at[k, m], tok_sem.at[k, m])
        keep("up", 2 * k + 4 * m, dot(tok_v[k, m], cot[...]))

    def tok(k, m):
        for c in range(2):
            tok_send(k, m, c).start()

    def forward():
        wait_bytes(cot_slot(2), cot_sem.at[2])
        cot_forward().start()

    def advance(c, d):
        f = p.flows[c]
        entries = f.incoming(d)
        if entries:
            wait_bytes(own[c].at[pl.ds(0, len(entries))], flow_got[c].at[d])
        rows = f.shape[1]
        step = 32

        def body(i, carry):
            at = pl.ds(pl.multiple_of(i * step, step), step)
            value = own[c][d, at, :].astype(jnp.float32)
            for e in entries:
                value = value + got[c][e, at, :].astype(jnp.float32)
            if d:
                own[c][d, at, :] = value.astype(jnp.bfloat16)
            else:
                to = pl.ds(pl.multiple_of(f.rows[0] + i * step, step), step)
                outs[f.out][to, f.cols[0] - f.out_col:f.cols[1] - f.out_col] = value
            return carry
        if entries:
            lax.fori_loop(0, rows // step, body, 0)
        if d:
            flow_copy(c, d).start()

    tasks = p.tasks()
    order = [tasks[i] for i in ORDER]
    downs = [t[1:] for t in order if t[0] == "down"]
    ups = [t[1:] for t in order if t[0] == "up"]

    for u, m in downs:
        grad_copy(u, m).start()
    for k, m in ups:
        tok_copy(k, m).start()

    barrier = pltpu.get_barrier_semaphore()
    peers = [twin, crossed] + peer
    for to in peers:
        pl.semaphore_signal(barrier, inc=1, device_id=to, device_id_type=MESH)
    pl.semaphore_wait(barrier, len(peers))

    cot_send(2, across)
    hid_swap().start()
    for u, m in downs[:4]:
        grad_swap(u, m).start()
    tok(1, 3)
    for u, m in downs[4:]:
        grad_swap(u, m).start()
    cot_send(1, twin)
    for k, m in ups:
        tok_swap(k, m).start()
    hid[0:T] = hidden[...]
    cot[0:T, 0:F] = gate_cot[...]
    cot[0:T, F:2 * F] = up_cot[...]

    run = {"tok": tok, "forward": forward, "down": down, "up": up, "advance": advance}
    for task in order:
        run[task[0]](*task[1:])

    hid_swap().wait_send()
    wait_bytes(cot.at[pl.ds(0, 2 * T)], cot_sem.at[0])
    cot_forward().wait_send()
    wait_bytes(grad_v.at[:, :, pl.ds(0, T)], swap_sent.at[0])
    wait_bytes(tok_v.at[:, :, pl.ds(0, T)], swap_sent.at[1])
    wait_bytes(tok_v.at[:, :, pl.ds(0, 2 * T)], swap_sent.at[2])
    for c, f in enumerate(p.flows):
        wait_bytes(own[c].at[pl.ds(1, f.shape[0] - 1)], flow_sent.at[c])


def activate(gate_pre, up_pre, hidden_grad):
    gate_val, up_val, grad_val = (a.astype(jnp.float32) for a in (gate_pre, up_pre, hidden_grad))
    sig = jax.nn.sigmoid(gate_val)
    act = gate_val * sig
    gate_cot = grad_val * up_val * sig * (1.0 + gate_val * (1.0 - sig))
    return tuple(a.astype(jnp.bfloat16) for a in (gate_cot, grad_val * act, act * up_val))


def exchange_on_device(p, tokens, out_grad, gate_pre, up_pre, hidden_grad):
    T, R, F, bf16 = p.tok, p.rows, p.hidden, jnp.bfloat16
    scratch = [
        pltpu.VMEM((2 * T, F), bf16),
        pltpu.VMEM((4 * T, 2 * F), bf16),
        pltpu.VMEM((2, 4, 4 * T, R), bf16),
        pltpu.VMEM((4, 4, 2 * T, R), bf16),
    ]
    scratch += [pltpu.VMEM(f.shape, bf16) for f in p.flows] * 2
    held = sum(2 * math.prod(ref.shape) for ref in scratch) + 4 * 3 * R * F + 2 * 3 * T * F
    dma = pltpu.SemaphoreType.DMA
    scratch += [dma((7,)), dma((4, 4)), dma((2, 4)), dma((3,)), dma((len(p.flows),))]
    scratch += [dma((f.shape[0] // 2,)) for f in p.flows]
    out = jax.ShapeDtypeStruct((R, F), jnp.float32)
    return pl.pallas_call(
        functools.partial(exchange_kernel, p),
        out_shape=(out, out, out),
        in_specs=[pl.BlockSpec(memory_space=pltpu.HBM)] * 2 + [pl.BlockSpec(memory_space=pltpu.VMEM)] * 3,
        out_specs=[pl.BlockSpec(memory_space=pltpu.VMEM)] * 3,
        scratch_shapes=scratch,
        compiler_params=pltpu.CompilerParams(
            collective_id=0, has_side_effects=True, vmem_limit_bytes=held + SPARE
        ),
    )(tokens, out_grad, *activate(gate_pre, up_pre, hidden_grad))


def on_device(n_batch, n_seq, tokens, out_grad, gate_pre, up_pre, hidden_grad):
    tok, width = tokens.shape
    hidden = gate_pre.shape[1]
    sizes = (n_batch, n_seq, tok, width, hidden)
    if Exchange.fits(*sizes):
        return exchange_on_device(
            Exchange(*sizes), tokens, out_grad, gate_pre, up_pre, hidden_grad
        )
    p = Plan(*sizes)
    C, R, bf16 = p.chips, p.rows, jnp.bfloat16
    scratch = [
        pltpu.VMEM((3, 2 * tok, hidden), bf16),
        pltpu.VMEM((2 * tok, 3 * hidden), bf16),
        pltpu.VMEM((p.n_groups, C, 2 * tok, p.block), bf16),
        pltpu.VMEM((p.n_groups, C, 2 * tok, p.block), bf16),
    ]
    sizes = [hi - lo for lo, hi in p.spans]
    scratch += [pltpu.VMEM((n_batch, C, R, size), bf16) for size in sizes]
    for cls, size in enumerate(sizes):
        slots = 1 if p.batch_first[cls] else n_batch
        scratch += [pltpu.VMEM((slots, C >> (j + 1), R, size), bf16) for j in range(p.seq_bits)]
    for cls, size in enumerate(sizes):
        blocks = C if p.batch_first[cls] else 1
        scratch += [pltpu.VMEM((n_batch >> (j + 1), blocks, R, size), bf16) for j in range(p.batch_bits)]
    n_cls = len(sizes)
    dma = pltpu.SemaphoreType.DMA
    scratch += [
        dma((3,)),
        dma((p.n_groups, 2)), dma((p.n_groups, 2)), dma((p.n_groups, 2)),
        dma((n_cls, 2 * p.seq_bits, n_batch)), dma((n_cls, 2 * p.seq_bits, n_batch)),
        dma((n_cls, p.batch_bits, n_batch // 2)), dma((n_cls, p.batch_bits, n_batch // 2)),
    ]
    out = jax.ShapeDtypeStruct((R, hidden), jnp.float32)
    return pl.pallas_call(
        functools.partial(kernel, p),
        out_shape=(out, out, out),
        in_specs=[pl.BlockSpec(memory_space=pltpu.HBM)] * 5,
        out_specs=[pl.BlockSpec(memory_space=pltpu.VMEM)] * 3,
        scratch_shapes=scratch,
        compiler_params=pltpu.CompilerParams(
            collective_id=0, has_side_effects=True, vmem_limit_bytes=67043328
        ),
    )(tokens, out_grad, gate_pre, up_pre, hidden_grad)


def solution(mesh):
    rows = P(("batch", "seq"), None)
    outs = P(("seq", "batch"), None)
    body = functools.partial(on_device, mesh.shape["batch"], mesh.shape["seq"])
    return jax.shard_map(
        body, mesh=mesh, in_specs=(rows,) * 5, out_specs=(outs,) * 3, check_vma=False
    )
```

```python
import functools
import math

import jax
import jax.numpy as jnp
from jax import lax
from jax.experimental import pallas as pl
from jax.experimental.pallas import tpu as pltpu
from jax.sharding import PartitionSpec as P

MESH = pl.DeviceIdType.MESH
LANES = 128


def bit_count(n):
    return n.bit_length() - 1


def flip(value, mask):
    out, bit = value, 1
    while bit <= mask:
        if mask & bit:
            out = out + bit * (1 - 2 * ((value // bit) % 2))
        bit *= 2
    return out


class Plan:
    def __init__(self, n_batch, n_seq, tok, width, hidden):
        self.n_batch, self.n_seq, self.tok, self.width, self.hidden = n_batch, n_seq, tok, width, hidden
        self.chips = n_seq // 2
        self.seq_bits, self.batch_bits = bit_count(self.chips), bit_count(n_batch)
        self.rows = width // (n_batch * n_seq)
        self.group = max(1, LANES // self.rows)
        self.block = self.group * self.rows
        self.n_groups = n_batch // self.group
        total = 3 * hidden
        units = total // LANES
        late = max(2, units // 6)
        early = (units - late) // 2
        cuts = [0, early, units - late, units - late // 2, units]
        self.spans = [(a * LANES, b * LANES) for a, b in zip(cuts[:-1], cuts[1:])]
        self.ascending = [True, False, True, False]
        self.batch_first = [False, False, True, True]

    def seq_bit(self, cls, stage):
        return stage if self.ascending[cls] else self.seq_bits - 1 - stage

    def position(self, cls, u):
        if not self.ascending[cls]:
            return u
        return sum(((u // (1 << i)) % 2) * (1 << (self.seq_bits - 1 - i)) for i in range(self.seq_bits))

    def pieces(self, lo, hi, step):
        out = []
        while lo < hi:
            end = min(hi, (lo // step + 1) * step)
            out.append((lo, end))
            lo = end
        return out


def low_bit(m):
    return (m & -m).bit_length() - 1


def kernel(plan, tokens, out_grad, gate_pre, up_pre, hidden_grad, out_gate, out_up, out_down, *scratch):
    p = plan
    T, R, M, C, NB = p.tok, p.rows, p.block, p.chips, p.n_batch
    n_cls, sb, bb = len(p.spans), p.seq_bits, p.batch_bits
    scratch = list(scratch)
    raw, hid, tok_v, grad_v = (scratch.pop(0) for _ in range(4))
    terms = [scratch.pop(0) for _ in range(n_cls)]
    seq_in = [[scratch.pop(0) for _ in range(sb)] for _ in range(n_cls)]
    batch_in = [[scratch.pop(0) for _ in range(bb)] for _ in range(n_cls)]
    raw_sem, load_sem, swap_sem, swap_out, seq_send, seq_recv, batch_send, batch_recv = scratch
    outs = (out_gate, out_up, out_down)

    b_me, s_me = lax.axis_index("batch"), lax.axis_index("seq")
    core, chip = s_me % 2, s_me // 2
    twin = (b_me, s_me + 1 - 2 * core)
    seq_peer = [(b_me, flip(s_me, 2 << i)) for i in range(sb)]
    batch_peer = [(flip(b_me, 1 << i), s_me) for i in range(bb)]

    pre = (gate_pre, up_pre, hidden_grad)
    for i, ref in enumerate(pre):
        pltpu.make_async_copy(ref, raw.at[i, pl.ds(0, T)], raw_sem.at[0]).start()

    def column(g, u, side):
        k = flip(chip, u)
        first = flip(b_me // p.group, g) * p.group
        return pl.multiple_of(((k * 2 + side) * NB + first) * R, M)

    sends = []
    groups = list(range(p.n_groups - 1, -1, -1))

    def load(g):
        for a, (src, dst) in enumerate(((tokens, tok_v), (out_grad, grad_v))):
            for u in range(C):
                pltpu.make_async_copy(
                    src.at[:, pl.ds(column(g, u, core), M)], dst.at[g, u, pl.ds(0, T)], load_sem.at[g, a]
                ).start()

    def swap(g):
        for a, (src, dst) in enumerate(((tokens, tok_v), (out_grad, grad_v))):
            for u in range(C):
                pltpu.make_async_remote_copy(
                    src_ref=src.at[:, pl.ds(column(g, u, 1 - core), M)],
                    dst_ref=dst.at[g, u, pl.ds(T, T)],
                    send_sem=swap_out.at[g, a],
                    recv_sem=swap_sem.at[g, a],
                    device_id=twin,
                    device_id_type=MESH,
                ).start()

    for g in groups:
        load(g)

    barrier = pltpu.get_barrier_semaphore()
    peers = [twin] + seq_peer + batch_peer
    for peer in peers:
        pl.semaphore_signal(barrier, inc=1, device_id=peer, device_id_type=MESH)
    pl.semaphore_wait(barrier, len(peers))

    for i, ref in enumerate(pre):
        pltpu.make_async_remote_copy(
            src_ref=ref, dst_ref=raw.at[i, pl.ds(T, T)], send_sem=raw_sem.at[1], recv_sem=raw_sem.at[2],
            device_id=twin, device_id_type=MESH,
        ).start()
    for g in groups:
        swap(g)

    def activate(side):
        step = 32
        def body(i, carry):
            at = pl.ds(pl.multiple_of(side * T + i * step, step), step)
            gate_val = raw[0, at, :].astype(jnp.float32)
            up_val = raw[1, at, :].astype(jnp.float32)
            grad_val = raw[2, at, :].astype(jnp.float32)
            sig = jax.nn.sigmoid(gate_val)
            act = gate_val * sig
            F = p.hidden
            hid[at, 0:F] = (grad_val * up_val * sig * (1.0 + gate_val * (1.0 - sig))).astype(jnp.bfloat16)
            hid[at, F:2 * F] = (grad_val * act).astype(jnp.bfloat16)
            hid[at, 2 * F:3 * F] = (act * up_val).astype(jnp.bfloat16)
            return carry
        lax.fori_loop(0, T // step, body, 0)

    def wait_bytes(ref, sem):
        pltpu.make_async_copy(ref, ref, sem).wait()

    wait_bytes(raw.at[:, pl.ds(0, T)], raw_sem.at[0])
    activate(0)
    wait_bytes(raw.at[:, pl.ds(T, T)], raw_sem.at[2])
    activate(1)

    def arrive(g):
        for a, dst in enumerate((tok_v, grad_v)):
            wait_bytes(dst.at[g, :, pl.ds(0, T)], load_sem.at[g, a])
            wait_bytes(dst.at[g, :, pl.ds(T, T)], swap_sem.at[g, a])

    def compute_block(g, u):
        feats, grads = tok_v[g, u], grad_v[g, u]
        for cls, (lo, hi) in enumerate(p.spans):
            pos = p.position(cls, u)
            for a, b in p.pieces(lo, hi, 2 * p.hidden):
                value = lax.dot_general(
                    feats if a < 2 * p.hidden else grads, hid[:, a:b],
                    (((0,), (0,)), ((), ())), preferred_element_type=jnp.float32,
                ).astype(jnp.bfloat16)
                for h in range(p.group):
                    m = g if p.group == 1 else g * p.group + flip(b_me % p.group, h)
                    terms[cls][m, pos, :, a - lo:b - lo] = value[h * R:(h + 1) * R]

    def compute(g):
        arrive(g)

        def body(u, carry):
            compute_block(g, u)
            return carry
        lax.fori_loop(0, C, body, 0)

    step = min(R, 32)

    def gather(cls, m, first, count, extra):
        def body(i, carry):
            blk, at = first + i // (R // step), pl.ds(pl.multiple_of((i % (R // step)) * step, step), step)
            value = terms[cls][m, blk, at, :].astype(jnp.float32)
            for ref, slot in extra:
                value = value + ref[slot, blk, at, :].astype(jnp.float32)
            terms[cls][m, blk, at, :] = value.astype(jnp.bfloat16)
            return carry
        if extra:
            lax.fori_loop(0, count * (R // step), body, 0)

    def finish(cls, extra):
        lo, hi = p.spans[cls]
        def body(i, carry):
            at = pl.ds(pl.multiple_of(i * step, step), step)
            for a, b in p.pieces(lo, hi, p.hidden):
                value = terms[cls][0, 0, at, a - lo:b - lo].astype(jnp.float32)
                for ref, slot in extra:
                    value = value + ref[slot, 0, at, a - lo:b - lo].astype(jnp.float32)
                base = (a // p.hidden) * p.hidden
                outs[a // p.hidden][at, a - base:b - base] = value
            return carry
        lax.fori_loop(0, R // step, body, 0)

    def seq_slot(cls, m):
        return 0 if p.batch_first[cls] else m

    def halves(stage):
        return 2 if C >> (stage + 1) > 1 else 1

    def seq_copy(cls, m, stage, part):
        count = C >> (stage + 1)
        size = count // halves(stage)
        first = count - size if part == 0 else 0
        slot = seq_slot(cls, m)
        return pltpu.make_async_remote_copy(
            src_ref=terms[cls].at[m, pl.ds(count + first, size)],
            dst_ref=seq_in[cls][stage].at[slot, pl.ds(first, size)],
            send_sem=seq_send.at[cls, 2 * stage + part, slot],
            recv_sem=seq_recv.at[cls, 2 * stage + part, slot],
            device_id=seq_peer[p.seq_bit(cls, stage)],
            device_id_type=MESH,
        )

    def batch_copy(cls, m):
        stage = low_bit(m)
        slot = m >> (stage + 1)
        count = C if p.batch_first[cls] else 1
        return pltpu.make_async_remote_copy(
            src_ref=terms[cls].at[m, pl.ds(0, count)],
            dst_ref=batch_in[cls][stage].at[slot],
            send_sem=batch_send.at[cls, stage, slot],
            recv_sem=batch_recv.at[cls, stage, slot],
            device_id=batch_peer[stage],
            device_id_type=MESH,
        )

    def start(copy):
        copy.start()
        sends.append(copy)

    def from_seq(cls, m, stages):
        return [(seq_in[cls][j], seq_slot(cls, m)) for j in range(stages)]

    def from_batch(cls, m):
        count = bb if m == 0 else low_bit(m)
        return [(batch_in[cls][j], m >> (j + 1)) for j in range(count)]

    def wait_batch(cls, m):
        count = bb if m == 0 else low_bit(m)
        for j in range(count):
            batch_copy(cls, m + (1 << j)).wait_recv()

    def wait_seq(cls, m, stage):
        if stage >= 0:
            seq_copy(cls, m, stage, 0).wait_recv()
        if stage >= 1:
            seq_copy(cls, m, stage - 1, 1).wait_recv()

    def seq_stage(cls, m, stage, base, parts=(0, 1)):
        wait_seq(cls, m, stage - 1)
        count = C >> (stage + 1)
        gather(cls, m, count, count, base + from_seq(cls, m, stage))
        for part in parts[:halves(stage)]:
            start(seq_copy(cls, m, stage, part))

    def batch_last(cls, m):
        wait_seq(cls, m, sb - 1)
        wait_batch(cls, m)
        extra = from_seq(cls, m, sb) + from_batch(cls, m)
        if m == 0:
            finish(cls, extra)
        else:
            gather(cls, m, 0, 1, extra)
            start(batch_copy(cls, m))

    def batch_early(cls, m):
        wait_batch(cls, m)
        if m:
            gather(cls, m, 0, C, from_batch(cls, m))
            start(batch_copy(cls, m))
        else:
            seq_stage(cls, 0, 0, from_batch(cls, 0))

    plain = [c for c in range(n_cls) if not p.batch_first[c]]
    early = [c for c in range(n_cls) if p.batch_first[c]]
    order = list(range(NB - 1, -1, -1))
    done = set()

    def need(i):
        if i < NB and order[i] // p.group not in done:
            done.add(order[i] // p.group)
            compute(order[i] // p.group)

    def first_round():
        g = groups[0]
        done.add(g)
        arrive(g)
        upper = [u for u in range(C) if any(p.position(c, u) >= C - C // 4 for c in plain)] if p.group == 1 else []
        for u in upper:
            compute_block(g, u)
        split = bool(upper) and halves(0) == 2
        if split:
            for cls in plain:
                start(seq_copy(cls, order[0], 0, 0))
        rest = [u for u in range(C) if u not in upper]
        if rest == list(range(len(rest))):
            def body(u, carry):
                compute_block(g, u)
                return carry
            lax.fori_loop(0, len(rest), body, 0)
        else:
            for u in rest:
                compute_block(g, u)
        for cls in plain:
            for part in range(1 if split else 0, halves(0)):
                start(seq_copy(cls, order[0], 0, part))
        if order[0] % 2:
            for cls in early:
                batch_early(cls, order[0])

    first_round()
    for i in range(1, NB + 1):
        before = order[i - 1]
        need(i)
        if i == 1:
            need(2)
        for stage in range(1, sb):
            for cls in plain:
                seq_stage(cls, before, stage, [])
        if i < NB:
            for cls in plain:
                seq_stage(cls, order[i], 0, [])
        if i + 1 < NB:
            need(i + 1)
        for cls in early:
            if i + 1 < NB and order[i + 1] % 2:
                batch_early(cls, order[i + 1])
            if i < NB and order[i] and order[i] % 2 == 0:
                batch_early(cls, order[i])
        if i == NB:
            for cls in early:
                batch_early(cls, 0)
        for cls in plain:
            batch_last(cls, before)
    for stage in range(1, sb):
        for cls in early:
            seq_stage(cls, 0, stage, from_batch(cls, 0))
    for cls in early:
        wait_seq(cls, 0, sb - 1)
        finish(cls, from_batch(cls, 0) + from_seq(cls, 0, sb))

    for copy in sends:
        copy.wait_send()
    wait_bytes(raw.at[:, pl.ds(T, T)], raw_sem.at[1])
    for g in groups:
        for a, dst in enumerate((tok_v, grad_v)):
            wait_bytes(dst.at[g, :, pl.ds(T, T)], swap_out.at[g, a])


X, Y, Z0, Z1 = range(4)


class Flow:
    def __init__(self, source, order, rows, cols, out, out_col):
        self.source, self.order, self.rows, self.cols = source, order, rows, cols
        self.out, self.out_col = out, out_col
        self.n = len(order)
        self.shape = (1 << self.n, rows[1] - rows[0], cols[1] - cols[0])

    def dense(self, block):
        return sum(((block >> b) & 1) << (self.n - 1 - i) for i, b in enumerate(self.order))

    def block(self, d):
        return sum(((d >> (self.n - 1 - i)) & 1) << b for i, b in enumerate(self.order))

    def stage(self, d):
        return self.n - d.bit_length()

    def incoming(self, d):
        return [d + (1 << (self.n - 1 - i)) for i in range(self.stage(d))]


class Exchange:
    def __init__(self, n_batch, n_seq, tok, width, hidden):
        self.n_batch, self.n_seq, self.tok, self.width, self.hidden = n_batch, n_seq, tok, width, hidden
        self.rows = R = width // (n_batch * n_seq)
        unit, half = hidden // 6, R // 2
        full = (0, R)
        batch_first, y_first, x_first = (Z0, Z1, X, Y), (Y, X, Z0, Z1), (X, Y, Z0, Z1)
        def up(a, b):
            out = a // 6
            return Flow("up", (Y, Z0, Z1), full, (a * unit, b * unit), out, out * hidden)
        def down(order, rows, a, b):
            return Flow("down", order, rows, (a * unit, b * unit), 2, 0)
        self.flows = [
            up(0, 3),
            up(3, 6),
            up(6, 9),
            up(9, 12),
            down(batch_first, full, 0, 2),
            down(batch_first, (0, half), 2, 3),
            down(x_first, (half, R), 2, 3),
            down(y_first, full, 3, 6),
        ]

    @staticmethod
    def fits(n_batch, n_seq, tok, width, hidden):
        return n_batch == 4 and n_seq == 8 and hidden % (6 * LANES) == 0 and width % (n_batch * n_seq * LANES) == 0

    def tasks(self):
        out = [("tok", k, m) for k in (1, 0) for m in (3, 1, 2, 0)]
        out += [("forward",)]
        out += [("down", u, m) for u in range(4) for m in range(4)]
        out += [("up", k, m) for k in range(2) for m in range(4)]
        out += [("advance", c, d) for c, f in enumerate(self.flows) for d in range(1 << f.n)]
        return out


SPARE = 6 << 20
ORDER = (
    24, 128, 96, 80, 16, 10, 21, 23, 22, 76, 13, 17, 126, 12, 18, 9,
    20, 72, 19, 123, 78, 77, 74, 88, 121, 127, 122, 14, 15, 70, 93, 79,
    92, 8, 11, 89, 125, 124, 69, 75, 120, 4, 32, 91, 48, 94, 95, 73,
    2, 116, 118, 40, 90, 56, 71, 28, 64, 86, 44, 6, 87, 31, 36, 1,
    46, 119, 85, 52, 114, 38, 54, 27, 42, 62, 60, 112, 5, 34, 30, 55,
    47, 63, 39, 3, 115, 50, 104, 117, 26, 43, 29, 110, 53, 7, 45, 35,
    58, 102, 107, 51, 108, 84, 37, 111, 68, 25, 106, 61, 67, 103, 109, 100,
    66, 82, 59, 33, 83, 98, 41, 101, 105, 99, 113, 49, 65, 81, 57, 97,
)


def exchange_kernel(plan, tokens, out_grad, gate_cot, up_cot, hidden, out, *scratch):
    p = plan
    T, R, F, NB = p.tok, p.rows, p.hidden, p.n_batch
    n_flows = len(p.flows)
    scratch = list(scratch)
    hid, cot, tok_v, grad_v = (scratch.pop(0) for _ in range(4))
    own = [scratch.pop(0) for _ in range(n_flows)]
    got = [scratch.pop(0) for _ in range(n_flows)]
    cot_sem, grad_sem, tok_sem, swap_sent, flow_sent = (scratch.pop(0) for _ in range(5))
    flow_got = scratch
    outs = [out.at[:, pl.ds(i * F, F)] for i in range(3)]

    b_me, s_me = lax.axis_index("batch"), lax.axis_index("seq")

    def device(block, other=0):
        return (flip(b_me, block >> 2), flip(s_me, 2 * (block & 3) + other))

    def columns(block, other=0):
        b, s = device(block, other)
        return pl.ds(pl.multiple_of((s * NB + b) * R, R), R)

    twin, across, crossed = device(0, 1), device(1 << X), device(1 << X, 1)
    peer = [device(1 << bit) for bit in range(4)]

    def remote(src, dst, send_sem, recv_sem, to):
        return pltpu.make_async_remote_copy(
            src_ref=src, dst_ref=dst, send_sem=send_sem, recv_sem=recv_sem, device_id=to, device_id_type=MESH
        )

    def wait_bytes(ref, sem):
        pltpu.make_async_copy(ref, ref, sem).wait()

    def grad_copy(u, m):
        return pltpu.make_async_copy(
            out_grad.at[:, columns(u + 4 * m)], grad_v.at[u, m, pl.ds(0, T)], grad_sem.at[u, m])

    def grad_swap(u, m):
        return remote(out_grad.at[:, columns(u + 4 * m, 1)], grad_v.at[u, m, pl.ds(T, T)],
                      swap_sent.at[0], grad_sem.at[u, m], twin)

    def tok_copy(k, m):
        return pltpu.make_async_copy(
            tokens.at[:, columns(2 * k + 4 * m)], tok_v.at[k, m, pl.ds(0, T)], tok_sem.at[k, m])

    def tok_swap(k, m):
        return remote(tokens.at[:, columns(2 * k + 4 * m, 1)], tok_v.at[k, m, pl.ds(T, T)],
                      swap_sent.at[1], tok_sem.at[k, m], twin)

    def tok_send(k, m, c):
        return remote(tokens.at[:, columns(1 + 2 * k + 4 * m, c)], tok_v.at[k, m, pl.ds((2 + c) * T, T)],
                      swap_sent.at[2], tok_sem.at[k, m], crossed if c else across)

    def cot_slot(slot):
        return cot.at[pl.ds(slot * T, T)]

    def cot_send(slot, to):
        for i, ref in enumerate((gate_cot, up_cot)):
            remote(ref, cot.at[pl.ds(slot * T, T), pl.ds(i * F, F)], cot_sem.at[0], cot_sem.at[slot], to).start()

    def cot_forward():
        return remote(cot_slot(2), cot_slot(3), cot_sem.at[4], cot_sem.at[3], twin)

    def hid_swap():
        return remote(hidden, hid.at[pl.ds(T, T)], cot_sem.at[5], cot_sem.at[6], twin)

    def flow_copy(c, d):
        f = p.flows[c]
        to = d - (1 << (f.n - 1 - f.stage(d)))
        return remote(own[c].at[d], got[c].at[d], flow_sent.at[c], flow_got[c].at[to], peer[f.order[f.stage(d)]])

    dot = functools.partial(
        lax.dot_general, dimension_numbers=(((0,), (0,)), ((), ())), preferred_element_type=jnp.float32)

    def keep(source, block, value):
        for c, f in enumerate(p.flows):
            if f.source == source:
                own[c][f.dense(block)] = value[f.rows[0]:f.rows[1], f.cols[0]:f.cols[1]].astype(jnp.bfloat16)

    waits = {"hid", "cot"}

    def down(u, m):
        if "hid" in waits:
            waits.remove("hid")
            hid_swap().wait_recv()
        wait_bytes(grad_v.at[u, m], grad_sem.at[u, m])
        keep("down", u + 4 * m, dot(grad_v[u, m], hid[...]))

    def up(k, m):
        if "cot" in waits:
            waits.remove("cot")
            wait_bytes(cot_slot(1), cot_sem.at[1])
            cot_forward().wait_recv()
        wait_bytes(tok_v.at[k, m], tok_sem.at[k, m])
        keep("up", 2 * k + 4 * m, dot(tok_v[k, m], cot[...]))

    def tok(k, m):
        for c in range(2):
            tok_send(k, m, c).start()

    def forward():
        wait_bytes(cot_slot(2), cot_sem.at[2])
        cot_forward().start()

    def advance(c, d):
        f = p.flows[c]
        entries = f.incoming(d)
        if entries:
            wait_bytes(own[c].at[pl.ds(0, len(entries))], flow_got[c].at[d])
        rows = f.shape[1]
        step = 32

        def body(i, carry):
            at = pl.ds(pl.multiple_of(i * step, step), step)
            value = own[c][d, at, :].astype(jnp.float32)
            for e in entries:
                value = value + got[c][e, at, :].astype(jnp.float32)
            if d:
                own[c][d, at, :] = value.astype(jnp.bfloat16)
            else:
                to = pl.ds(pl.multiple_of(f.rows[0] + i * step, step), step)
                outs[f.out][to, f.cols[0] - f.out_col:f.cols[1] - f.out_col] = value
            return carry
        if entries:
            lax.fori_loop(0, rows // step, body, 0)
        if d:
            flow_copy(c, d).start()

    tasks = p.tasks()
    order = [tasks[i] for i in ORDER]
    downs = [t[1:] for t in order if t[0] == "down"]
    ups = [t[1:] for t in order if t[0] == "up"]

    for u, m in downs:
        grad_copy(u, m).start()
    for k, m in ups:
        tok_copy(k, m).start()

    barrier = pltpu.get_barrier_semaphore()
    peers = [twin, crossed] + peer
    for to in peers:
        pl.semaphore_signal(barrier, inc=1, device_id=to, device_id_type=MESH)
    pl.semaphore_wait(barrier, len(peers))

    cot_send(2, across)
    hid_swap().start()
    for u, m in downs[:4]:
        grad_swap(u, m).start()
    tok(1, 3)
    for u, m in downs[4:]:
        grad_swap(u, m).start()
    cot_send(1, twin)
    for k, m in ups:
        tok_swap(k, m).start()
    hid[0:T] = hidden[...]
    cot[0:T, 0:F] = gate_cot[...]
    cot[0:T, F:2 * F] = up_cot[...]

    run = {"tok": tok, "forward": forward, "down": down, "up": up, "advance": advance}
    for task in order:
        run[task[0]](*task[1:])

    hid_swap().wait_send()
    wait_bytes(cot.at[pl.ds(0, 2 * T)], cot_sem.at[0])
    cot_forward().wait_send()
    wait_bytes(grad_v.at[:, :, pl.ds(0, T)], swap_sent.at[0])
    wait_bytes(tok_v.at[:, :, pl.ds(0, T)], swap_sent.at[1])
    wait_bytes(tok_v.at[:, :, pl.ds(0, 2 * T)], swap_sent.at[2])
    for c, f in enumerate(p.flows):
        wait_bytes(own[c].at[pl.ds(1, f.shape[0] - 1)], flow_sent.at[c])


def activate(gate_pre, up_pre, hidden_grad):
    gate_val, up_val, grad_val = (a.astype(jnp.float32) for a in (gate_pre, up_pre, hidden_grad))
    sig = jax.nn.sigmoid(gate_val)
    act = gate_val * sig
    gate_cot = grad_val * up_val * sig * (1.0 + gate_val * (1.0 - sig))
    return tuple(a.astype(jnp.bfloat16) for a in (gate_cot, grad_val * act, act * up_val))


def exchange_on_device(p, tokens, out_grad, gate_pre, up_pre, hidden_grad):
    T, R, F, bf16 = p.tok, p.rows, p.hidden, jnp.bfloat16
    scratch = [
        pltpu.VMEM((2 * T, F), bf16),
        pltpu.VMEM((4 * T, 2 * F), bf16),
        pltpu.VMEM((2, 4, 4 * T, R), bf16),
        pltpu.VMEM((4, 4, 2 * T, R), bf16),
    ]
    scratch += [pltpu.VMEM(f.shape, bf16) for f in p.flows] * 2
    held = sum(2 * math.prod(ref.shape) for ref in scratch) + 4 * 3 * R * F + 2 * 3 * T * F
    dma = pltpu.SemaphoreType.DMA
    scratch += [dma((7,)), dma((4, 4)), dma((2, 4)), dma((3,)), dma((len(p.flows),))]
    scratch += [dma((f.shape[0] // 2,)) for f in p.flows]
    out = pl.pallas_call(
        functools.partial(exchange_kernel, p),
        out_shape=jax.ShapeDtypeStruct((R, 3 * F), jnp.float32),
        in_specs=[pl.BlockSpec(memory_space=pltpu.HBM)] * 2 + [pl.BlockSpec(memory_space=pltpu.VMEM)] * 3,
        out_specs=pl.BlockSpec(memory_space=pltpu.VMEM),
        scratch_shapes=scratch,
        compiler_params=pltpu.CompilerParams(
            collective_id=0, has_side_effects=True, vmem_limit_bytes=held + SPARE
        ),
    )(tokens, out_grad, *activate(gate_pre, up_pre, hidden_grad))
    return out[:, :F], out[:, F:2 * F], out[:, 2 * F:]


def on_device(n_batch, n_seq, tokens, out_grad, gate_pre, up_pre, hidden_grad):
    tok, width = tokens.shape
    hidden = gate_pre.shape[1]
    sizes = (n_batch, n_seq, tok, width, hidden)
    if Exchange.fits(*sizes):
        return exchange_on_device(
            Exchange(*sizes), tokens, out_grad, gate_pre, up_pre, hidden_grad
        )
    p = Plan(*sizes)
    C, R, bf16 = p.chips, p.rows, jnp.bfloat16
    scratch = [
        pltpu.VMEM((3, 2 * tok, hidden), bf16),
        pltpu.VMEM((2 * tok, 3 * hidden), bf16),
        pltpu.VMEM((p.n_groups, C, 2 * tok, p.block), bf16),
        pltpu.VMEM((p.n_groups, C, 2 * tok, p.block), bf16),
    ]
    sizes = [hi - lo for lo, hi in p.spans]
    scratch += [pltpu.VMEM((n_batch, C, R, size), bf16) for size in sizes]
    for cls, size in enumerate(sizes):
        slots = 1 if p.batch_first[cls] else n_batch
        scratch += [pltpu.VMEM((slots, C >> (j + 1), R, size), bf16) for j in range(p.seq_bits)]
    for cls, size in enumerate(sizes):
        blocks = C if p.batch_first[cls] else 1
        scratch += [pltpu.VMEM((n_batch >> (j + 1), blocks, R, size), bf16) for j in range(p.batch_bits)]
    n_cls = len(sizes)
    dma = pltpu.SemaphoreType.DMA
    scratch += [
        dma((3,)),
        dma((p.n_groups, 2)), dma((p.n_groups, 2)), dma((p.n_groups, 2)),
        dma((n_cls, 2 * p.seq_bits, n_batch)), dma((n_cls, 2 * p.seq_bits, n_batch)),
        dma((n_cls, p.batch_bits, n_batch // 2)), dma((n_cls, p.batch_bits, n_batch // 2)),
    ]
    out = jax.ShapeDtypeStruct((R, hidden), jnp.float32)
    return pl.pallas_call(
        functools.partial(kernel, p),
        out_shape=(out, out, out),
        in_specs=[pl.BlockSpec(memory_space=pltpu.HBM)] * 5,
        out_specs=[pl.BlockSpec(memory_space=pltpu.VMEM)] * 3,
        scratch_shapes=scratch,
        compiler_params=pltpu.CompilerParams(
            collective_id=0, has_side_effects=True, vmem_limit_bytes=67043328
        ),
    )(tokens, out_grad, gate_pre, up_pre, hidden_grad)


def solution(mesh):
    rows = P(("batch", "seq"), None)
    outs = P(("seq", "batch"), None)
    body = functools.partial(on_device, mesh.shape["batch"], mesh.shape["seq"])
    return jax.shard_map(
        body, mesh=mesh, in_specs=(rows,) * 5, out_specs=(outs,) * 3, check_vma=False
    )
```

```python
import functools
import math

import jax
import jax.numpy as jnp
from jax import lax
from jax.experimental import pallas as pl
from jax.experimental.pallas import tpu as pltpu
from jax.sharding import PartitionSpec as P

MESH = pl.DeviceIdType.MESH
LANES = 128


def bit_count(n):
    return n.bit_length() - 1


def flip(value, mask):
    out, bit = value, 1
    while bit <= mask:
        if mask & bit:
            out = out + bit * (1 - 2 * ((value // bit) % 2))
        bit *= 2
    return out


class Plan:
    def __init__(self, n_batch, n_seq, tok, width, hidden):
        self.n_batch, self.n_seq, self.tok, self.width, self.hidden = n_batch, n_seq, tok, width, hidden
        self.chips = n_seq // 2
        self.seq_bits, self.batch_bits = bit_count(self.chips), bit_count(n_batch)
        self.rows = width // (n_batch * n_seq)
        self.group = max(1, LANES // self.rows)
        self.block = self.group * self.rows
        self.n_groups = n_batch // self.group
        total = 3 * hidden
        units = total // LANES
        late = max(2, units // 6)
        early = (units - late) // 2
        cuts = [0, early, units - late, units - late // 2, units]
        self.spans = [(a * LANES, b * LANES) for a, b in zip(cuts[:-1], cuts[1:])]
        self.ascending = [True, False, True, False]
        self.batch_first = [False, False, True, True]

    def seq_bit(self, cls, stage):
        return stage if self.ascending[cls] else self.seq_bits - 1 - stage

    def position(self, cls, u):
        if not self.ascending[cls]:
            return u
        return sum(((u // (1 << i)) % 2) * (1 << (self.seq_bits - 1 - i)) for i in range(self.seq_bits))

    def pieces(self, lo, hi, step):
        out = []
        while lo < hi:
            end = min(hi, (lo // step + 1) * step)
            out.append((lo, end))
            lo = end
        return out


def low_bit(m):
    return (m & -m).bit_length() - 1


def kernel(plan, tokens, out_grad, gate_pre, up_pre, hidden_grad, out_gate, out_up, out_down, *scratch):
    p = plan
    T, R, M, C, NB = p.tok, p.rows, p.block, p.chips, p.n_batch
    n_cls, sb, bb = len(p.spans), p.seq_bits, p.batch_bits
    scratch = list(scratch)
    raw, hid, tok_v, grad_v = (scratch.pop(0) for _ in range(4))
    terms = [scratch.pop(0) for _ in range(n_cls)]
    seq_in = [[scratch.pop(0) for _ in range(sb)] for _ in range(n_cls)]
    batch_in = [[scratch.pop(0) for _ in range(bb)] for _ in range(n_cls)]
    raw_sem, load_sem, swap_sem, swap_out, seq_send, seq_recv, batch_send, batch_recv = scratch
    outs = (out_gate, out_up, out_down)

    b_me, s_me = lax.axis_index("batch"), lax.axis_index("seq")
    core, chip = s_me % 2, s_me // 2
    twin = (b_me, s_me + 1 - 2 * core)
    seq_peer = [(b_me, flip(s_me, 2 << i)) for i in range(sb)]
    batch_peer = [(flip(b_me, 1 << i), s_me) for i in range(bb)]

    pre = (gate_pre, up_pre, hidden_grad)
    for i, ref in enumerate(pre):
        pltpu.make_async_copy(ref, raw.at[i, pl.ds(0, T)], raw_sem.at[0]).start()

    def column(g, u, side):
        k = flip(chip, u)
        first = flip(b_me // p.group, g) * p.group
        return pl.multiple_of(((k * 2 + side) * NB + first) * R, M)

    sends = []
    groups = list(range(p.n_groups - 1, -1, -1))

    def load(g):
        for a, (src, dst) in enumerate(((tokens, tok_v), (out_grad, grad_v))):
            for u in range(C):
                pltpu.make_async_copy(
                    src.at[:, pl.ds(column(g, u, core), M)], dst.at[g, u, pl.ds(0, T)], load_sem.at[g, a]
                ).start()

    def swap(g):
        for a, (src, dst) in enumerate(((tokens, tok_v), (out_grad, grad_v))):
            for u in range(C):
                pltpu.make_async_remote_copy(
                    src_ref=src.at[:, pl.ds(column(g, u, 1 - core), M)],
                    dst_ref=dst.at[g, u, pl.ds(T, T)],
                    send_sem=swap_out.at[g, a],
                    recv_sem=swap_sem.at[g, a],
                    device_id=twin,
                    device_id_type=MESH,
                ).start()

    for g in groups:
        load(g)

    barrier = pltpu.get_barrier_semaphore()
    peers = [twin] + seq_peer + batch_peer
    for peer in peers:
        pl.semaphore_signal(barrier, inc=1, device_id=peer, device_id_type=MESH)
    pl.semaphore_wait(barrier, len(peers))

    for i, ref in enumerate(pre):
        pltpu.make_async_remote_copy(
            src_ref=ref, dst_ref=raw.at[i, pl.ds(T, T)], send_sem=raw_sem.at[1], recv_sem=raw_sem.at[2],
            device_id=twin, device_id_type=MESH,
        ).start()
    for g in groups:
        swap(g)

    def activate(side):
        step = 32
        def body(i, carry):
            at = pl.ds(pl.multiple_of(side * T + i * step, step), step)
            gate_val = raw[0, at, :].astype(jnp.float32)
            up_val = raw[1, at, :].astype(jnp.float32)
            grad_val = raw[2, at, :].astype(jnp.float32)
            sig = jax.nn.sigmoid(gate_val)
            act = gate_val * sig
            F = p.hidden
            hid[at, 0:F] = (grad_val * up_val * sig * (1.0 + gate_val * (1.0 - sig))).astype(jnp.bfloat16)
            hid[at, F:2 * F] = (grad_val * act).astype(jnp.bfloat16)
            hid[at, 2 * F:3 * F] = (act * up_val).astype(jnp.bfloat16)
            return carry
        lax.fori_loop(0, T // step, body, 0)

    def wait_bytes(ref, sem):
        pltpu.make_async_copy(ref, ref, sem).wait()

    wait_bytes(raw.at[:, pl.ds(0, T)], raw_sem.at[0])
    activate(0)
    wait_bytes(raw.at[:, pl.ds(T, T)], raw_sem.at[2])
    activate(1)

    def arrive(g):
        for a, dst in enumerate((tok_v, grad_v)):
            wait_bytes(dst.at[g, :, pl.ds(0, T)], load_sem.at[g, a])
            wait_bytes(dst.at[g, :, pl.ds(T, T)], swap_sem.at[g, a])

    def compute_block(g, u):
        feats, grads = tok_v[g, u], grad_v[g, u]
        for cls, (lo, hi) in enumerate(p.spans):
            pos = p.position(cls, u)
            for a, b in p.pieces(lo, hi, 2 * p.hidden):
                value = lax.dot_general(
                    feats if a < 2 * p.hidden else grads, hid[:, a:b],
                    (((0,), (0,)), ((), ())), preferred_element_type=jnp.float32,
                ).astype(jnp.bfloat16)
                for h in range(p.group):
                    m = g if p.group == 1 else g * p.group + flip(b_me % p.group, h)
                    terms[cls][m, pos, :, a - lo:b - lo] = value[h * R:(h + 1) * R]

    def compute(g):
        arrive(g)

        def body(u, carry):
            compute_block(g, u)
            return carry
        lax.fori_loop(0, C, body, 0)

    step = min(R, 32)

    def gather(cls, m, first, count, extra):
        def body(i, carry):
            blk, at = first + i // (R // step), pl.ds(pl.multiple_of((i % (R // step)) * step, step), step)
            value = terms[cls][m, blk, at, :].astype(jnp.float32)
            for ref, slot in extra:
                value = value + ref[slot, blk, at, :].astype(jnp.float32)
            terms[cls][m, blk, at, :] = value.astype(jnp.bfloat16)
            return carry
        if extra:
            lax.fori_loop(0, count * (R // step), body, 0)

    def finish(cls, extra):
        lo, hi = p.spans[cls]
        def body(i, carry):
            at = pl.ds(pl.multiple_of(i * step, step), step)
            for a, b in p.pieces(lo, hi, p.hidden):
                value = terms[cls][0, 0, at, a - lo:b - lo].astype(jnp.float32)
                for ref, slot in extra:
                    value = value + ref[slot, 0, at, a - lo:b - lo].astype(jnp.float32)
                base = (a // p.hidden) * p.hidden
                outs[a // p.hidden][at, a - base:b - base] = value
            return carry
        lax.fori_loop(0, R // step, body, 0)

    def seq_slot(cls, m):
        return 0 if p.batch_first[cls] else m

    def halves(stage):
        return 2 if C >> (stage + 1) > 1 else 1

    def seq_copy(cls, m, stage, part):
        count = C >> (stage + 1)
        size = count // halves(stage)
        first = count - size if part == 0 else 0
        slot = seq_slot(cls, m)
        return pltpu.make_async_remote_copy(
            src_ref=terms[cls].at[m, pl.ds(count + first, size)],
            dst_ref=seq_in[cls][stage].at[slot, pl.ds(first, size)],
            send_sem=seq_send.at[cls, 2 * stage + part, slot],
            recv_sem=seq_recv.at[cls, 2 * stage + part, slot],
            device_id=seq_peer[p.seq_bit(cls, stage)],
            device_id_type=MESH,
        )

    def batch_copy(cls, m):
        stage = low_bit(m)
        slot = m >> (stage + 1)
        count = C if p.batch_first[cls] else 1
        return pltpu.make_async_remote_copy(
            src_ref=terms[cls].at[m, pl.ds(0, count)],
            dst_ref=batch_in[cls][stage].at[slot],
            send_sem=batch_send.at[cls, stage, slot],
            recv_sem=batch_recv.at[cls, stage, slot],
            device_id=batch_peer[stage],
            device_id_type=MESH,
        )

    def start(copy):
        copy.start()
        sends.append(copy)

    def from_seq(cls, m, stages):
        return [(seq_in[cls][j], seq_slot(cls, m)) for j in range(stages)]

    def from_batch(cls, m):
        count = bb if m == 0 else low_bit(m)
        return [(batch_in[cls][j], m >> (j + 1)) for j in range(count)]

    def wait_batch(cls, m):
        count = bb if m == 0 else low_bit(m)
        for j in range(count):
            batch_copy(cls, m + (1 << j)).wait_recv()

    def wait_seq(cls, m, stage):
        if stage >= 0:
            seq_copy(cls, m, stage, 0).wait_recv()
        if stage >= 1:
            seq_copy(cls, m, stage - 1, 1).wait_recv()

    def seq_stage(cls, m, stage, base, parts=(0, 1)):
        wait_seq(cls, m, stage - 1)
        count = C >> (stage + 1)
        gather(cls, m, count, count, base + from_seq(cls, m, stage))
        for part in parts[:halves(stage)]:
            start(seq_copy(cls, m, stage, part))

    def batch_last(cls, m):
        wait_seq(cls, m, sb - 1)
        wait_batch(cls, m)
        extra = from_seq(cls, m, sb) + from_batch(cls, m)
        if m == 0:
            finish(cls, extra)
        else:
            gather(cls, m, 0, 1, extra)
            start(batch_copy(cls, m))

    def batch_early(cls, m):
        wait_batch(cls, m)
        if m:
            gather(cls, m, 0, C, from_batch(cls, m))
            start(batch_copy(cls, m))
        else:
            seq_stage(cls, 0, 0, from_batch(cls, 0))

    plain = [c for c in range(n_cls) if not p.batch_first[c]]
    early = [c for c in range(n_cls) if p.batch_first[c]]
    order = list(range(NB - 1, -1, -1))
    done = set()

    def need(i):
        if i < NB and order[i] // p.group not in done:
            done.add(order[i] // p.group)
            compute(order[i] // p.group)

    def first_round():
        g = groups[0]
        done.add(g)
        arrive(g)
        upper = [u for u in range(C) if any(p.position(c, u) >= C - C // 4 for c in plain)] if p.group == 1 else []
        for u in upper:
            compute_block(g, u)
        split = bool(upper) and halves(0) == 2
        if split:
            for cls in plain:
                start(seq_copy(cls, order[0], 0, 0))
        rest = [u for u in range(C) if u not in upper]
        if rest == list(range(len(rest))):
            def body(u, carry):
                compute_block(g, u)
                return carry
            lax.fori_loop(0, len(rest), body, 0)
        else:
            for u in rest:
                compute_block(g, u)
        for cls in plain:
            for part in range(1 if split else 0, halves(0)):
                start(seq_copy(cls, order[0], 0, part))
        if order[0] % 2:
            for cls in early:
                batch_early(cls, order[0])

    first_round()
    for i in range(1, NB + 1):
        before = order[i - 1]
        need(i)
        if i == 1:
            need(2)
        for stage in range(1, sb):
            for cls in plain:
                seq_stage(cls, before, stage, [])
        if i < NB:
            for cls in plain:
                seq_stage(cls, order[i], 0, [])
        if i + 1 < NB:
            need(i + 1)
        for cls in early:
            if i + 1 < NB and order[i + 1] % 2:
                batch_early(cls, order[i + 1])
            if i < NB and order[i] and order[i] % 2 == 0:
                batch_early(cls, order[i])
        if i == NB:
            for cls in early:
                batch_early(cls, 0)
        for cls in plain:
            batch_last(cls, before)
    for stage in range(1, sb):
        for cls in early:
            seq_stage(cls, 0, stage, from_batch(cls, 0))
    for cls in early:
        wait_seq(cls, 0, sb - 1)
        finish(cls, from_batch(cls, 0) + from_seq(cls, 0, sb))

    for copy in sends:
        copy.wait_send()
    wait_bytes(raw.at[:, pl.ds(T, T)], raw_sem.at[1])
    for g in groups:
        for a, dst in enumerate((tok_v, grad_v)):
            wait_bytes(dst.at[g, :, pl.ds(T, T)], swap_out.at[g, a])


X, Y, Z0, Z1 = range(4)


class Flow:
    def __init__(self, source, order, rows, cols, out, out_col):
        self.source, self.order, self.rows, self.cols = source, order, rows, cols
        self.out, self.out_col = out, out_col
        self.n = len(order)
        self.shape = (1 << self.n, rows[1] - rows[0], cols[1] - cols[0])

    def dense(self, block):
        return sum(((block >> b) & 1) << (self.n - 1 - i) for i, b in enumerate(self.order))

    def block(self, d):
        return sum(((d >> (self.n - 1 - i)) & 1) << b for i, b in enumerate(self.order))

    def stage(self, d):
        return self.n - d.bit_length()

    def incoming(self, d):
        return [d + (1 << (self.n - 1 - i)) for i in range(self.stage(d))]


class Exchange:
    def __init__(self, n_batch, n_seq, tok, width, hidden):
        self.n_batch, self.n_seq, self.tok, self.width, self.hidden = n_batch, n_seq, tok, width, hidden
        self.rows = R = width // (n_batch * n_seq)
        unit, half = hidden // 6, R // 2
        full = (0, R)
        batch_first, y_first, x_first = (Z0, Z1, X, Y), (Y, X, Z0, Z1), (X, Y, Z0, Z1)
        def up(a, b):
            out = a // 6
            return Flow("up", (Y, Z0, Z1), full, (a * unit, b * unit), out, out * hidden)
        def down(order, rows, a, b):
            return Flow("down", order, rows, (a * unit, b * unit), 2, 0)
        self.flows = [
            up(0, 3),
            up(3, 6),
            up(6, 9),
            up(9, 12),
            down(batch_first, full, 0, 2),
            down(batch_first, (0, half), 2, 3),
            down(x_first, (half, R), 2, 3),
            down(y_first, full, 3, 6),
        ]

    @staticmethod
    def fits(n_batch, n_seq, tok, width, hidden):
        return n_batch == 4 and n_seq == 8 and hidden % (6 * LANES) == 0 and width % (n_batch * n_seq * LANES) == 0

    def tasks(self):
        out = [("tok", k, m) for k in (1, 0) for m in (3, 1, 2, 0)]
        out += [("forward",)]
        out += [("down", u, m) for u in range(4) for m in range(4)]
        out += [("up", k, m) for k in range(2) for m in range(4)]
        out += [("advance", c, d) for c, f in enumerate(self.flows) for d in range(1 << f.n)]
        return out


SPARE = 6 << 20
ORDER = (
    20, 124, 78, 19, 24, 22, 23, 127, 122, 12, 80, 17, 70, 11, 77, 16,
    21, 128, 79, 69, 14, 121, 93, 75, 85, 18, 10, 92, 72, 15, 123, 96,
    74, 8, 71, 4, 94, 6, 126, 76, 125, 89, 95, 32, 56, 2, 90, 48,
    112, 73, 28, 91, 52, 86, 40, 88, 9, 120, 44, 64, 31, 36, 46, 27,
    1, 116, 119, 60, 87, 38, 5, 110, 54, 42, 34, 30, 111, 55, 104, 13,
    118, 3, 47, 39, 62, 50, 108, 115, 63, 26, 51, 114, 58, 109, 84, 103,
    29, 7, 102, 53, 35, 43, 45, 106, 68, 117, 100, 37, 105, 66, 59, 107,
    67, 61, 25, 33, 113, 82, 99, 83, 49, 98, 101, 65, 41, 57, 81, 97,
)


def exchange_kernel(plan, tokens, out_grad, gate_cot, up_cot, hidden, out, *scratch):
    p = plan
    T, R, F, NB = p.tok, p.rows, p.hidden, p.n_batch
    n_flows = len(p.flows)
    scratch = list(scratch)
    hid, cot, tok_v, grad_v = (scratch.pop(0) for _ in range(4))
    own = [scratch.pop(0) for _ in range(n_flows)]
    got = [scratch.pop(0) for _ in range(n_flows)]
    cot_sem, grad_sem, tok_sem, swap_sent, flow_sent = (scratch.pop(0) for _ in range(5))
    flow_got = scratch
    outs = [out.at[:, pl.ds(i * F, F)] for i in range(3)]

    b_me, s_me = lax.axis_index("batch"), lax.axis_index("seq")

    def device(block, other=0):
        return (flip(b_me, block >> 2), flip(s_me, 2 * (block & 3) + other))

    def columns(block, other=0):
        b, s = device(block, other)
        return pl.ds(pl.multiple_of((s * NB + b) * R, R), R)

    twin, across, crossed = device(0, 1), device(1 << X), device(1 << X, 1)
    peer = [device(1 << bit) for bit in range(4)]

    def remote(src, dst, send_sem, recv_sem, to):
        return pltpu.make_async_remote_copy(
            src_ref=src, dst_ref=dst, send_sem=send_sem, recv_sem=recv_sem, device_id=to, device_id_type=MESH
        )

    def wait_bytes(ref, sem):
        pltpu.make_async_copy(ref, ref, sem).wait()

    def grad_copy(u, m):
        return pltpu.make_async_copy(
            out_grad.at[:, columns(u + 4 * m)], grad_v.at[u, m, pl.ds(0, T)], grad_sem.at[u, m])

    def grad_swap(u, m):
        return remote(out_grad.at[:, columns(u + 4 * m, 1)], grad_v.at[u, m, pl.ds(T, T)],
                      swap_sent.at[0], grad_sem.at[u, m], twin)

    def tok_copy(k, m):
        return pltpu.make_async_copy(
            tokens.at[:, columns(2 * k + 4 * m)], tok_v.at[k, m, pl.ds(0, T)], tok_sem.at[k, m])

    def tok_swap(k, m):
        return remote(tokens.at[:, columns(2 * k + 4 * m, 1)], tok_v.at[k, m, pl.ds(T, T)],
                      swap_sent.at[1], tok_sem.at[k, m], twin)

    def tok_send(k, m, c):
        return remote(tokens.at[:, columns(1 + 2 * k + 4 * m, c)], tok_v.at[k, m, pl.ds((2 + c) * T, T)],
                      swap_sent.at[2], tok_sem.at[k, m], crossed if c else across)

    def cot_slot(slot):
        return cot.at[pl.ds(slot * T, T)]

    def cot_send(slot, to):
        for i, ref in enumerate((gate_cot, up_cot)):
            remote(ref, cot.at[pl.ds(slot * T, T), pl.ds(i * F, F)], cot_sem.at[0], cot_sem.at[slot], to).start()

    def cot_forward():
        return remote(cot_slot(2), cot_slot(3), cot_sem.at[4], cot_sem.at[3], twin)

    def hid_swap():
        return remote(hidden, hid.at[pl.ds(T, T)], cot_sem.at[5], cot_sem.at[6], twin)

    def flow_copy(c, d):
        f = p.flows[c]
        to = d - (1 << (f.n - 1 - f.stage(d)))
        return remote(own[c].at[d], got[c].at[d], flow_sent.at[c], flow_got[c].at[to], peer[f.order[f.stage(d)]])

    dot = functools.partial(
        lax.dot_general, dimension_numbers=(((0,), (0,)), ((), ())), preferred_element_type=jnp.float32)

    def keep(source, block, value):
        for c, f in enumerate(p.flows):
            if f.source == source:
                own[c][f.dense(block)] = value[f.rows[0]:f.rows[1], f.cols[0]:f.cols[1]].astype(jnp.bfloat16)

    waits = {"hid", "cot"}

    def down(u, m):
        if "hid" in waits:
            waits.remove("hid")
            hid_swap().wait_recv()
        wait_bytes(grad_v.at[u, m], grad_sem.at[u, m])
        keep("down", u + 4 * m, dot(grad_v[u, m], hid[...]))

    def up(k, m):
        if "cot" in waits:
            waits.remove("cot")
            wait_bytes(cot_slot(1), cot_sem.at[1])
            cot_forward().wait_recv()
        wait_bytes(tok_v.at[k, m], tok_sem.at[k, m])
        keep("up", 2 * k + 4 * m, dot(tok_v[k, m], cot[...]))

    def tok(k, m):
        for c in range(2):
            tok_send(k, m, c).start()

    def forward():
        wait_bytes(cot_slot(2), cot_sem.at[2])
        cot_forward().start()

    def advance(c, d):
        f = p.flows[c]
        entries = f.incoming(d)
        if entries:
            wait_bytes(own[c].at[pl.ds(0, len(entries))], flow_got[c].at[d])
        rows = f.shape[1]
        step = 32

        def body(i, carry):
            at = pl.ds(pl.multiple_of(i * step, step), step)
            value = own[c][d, at, :].astype(jnp.float32)
            for e in entries:
                value = value + got[c][e, at, :].astype(jnp.float32)
            if d:
                own[c][d, at, :] = value.astype(jnp.bfloat16)
            else:
                to = pl.ds(pl.multiple_of(f.rows[0] + i * step, step), step)
                outs[f.out][to, f.cols[0] - f.out_col:f.cols[1] - f.out_col] = value
            return carry
        if entries:
            lax.fori_loop(0, rows // step, body, 0)
        if d:
            flow_copy(c, d).start()

    tasks = p.tasks()
    order = [tasks[i] for i in ORDER]
    downs = [t[1:] for t in order if t[0] == "down"]
    ups = [t[1:] for t in order if t[0] == "up"]

    barrier = pltpu.get_barrier_semaphore()
    peers = [twin, crossed] + peer
    for to in peers[::-1]:
        pl.semaphore_signal(barrier, inc=1, device_id=to, device_id_type=MESH)
    for u, m in downs:
        grad_copy(u, m).start()
    for k, m in ups:
        tok_copy(k, m).start()
    hid[0:T] = hidden[...]
    cot[0:T, 0:F] = gate_cot[...]
    cot[0:T, F:2 * F] = up_cot[...]
    pl.semaphore_wait(barrier, len(peers))

    cot_send(2, across)
    hid_swap().start()
    for u, m in downs[:4]:
        grad_swap(u, m).start()
    tok(1, 3)
    for u, m in downs[4:]:
        grad_swap(u, m).start()
    cot_send(1, twin)
    for k, m in ups:
        tok_swap(k, m).start()

    run = {"tok": tok, "forward": forward, "down": down, "up": up, "advance": advance}
    for task in order:
        run[task[0]](*task[1:])

    hid_swap().wait_send()
    wait_bytes(cot.at[pl.ds(0, 2 * T)], cot_sem.at[0])
    cot_forward().wait_send()
    wait_bytes(grad_v.at[:, :, pl.ds(0, T)], swap_sent.at[0])
    wait_bytes(tok_v.at[:, :, pl.ds(0, T)], swap_sent.at[1])
    wait_bytes(tok_v.at[:, :, pl.ds(0, 2 * T)], swap_sent.at[2])
    for c, f in enumerate(p.flows):
        wait_bytes(own[c].at[pl.ds(1, f.shape[0] - 1)], flow_sent.at[c])


def activate(gate_pre, up_pre, hidden_grad):
    gate_val, up_val, grad_val = (a.astype(jnp.float32) for a in (gate_pre, up_pre, hidden_grad))
    sig = jax.nn.sigmoid(gate_val)
    act = gate_val * sig
    gate_cot = grad_val * up_val * sig * (1.0 + gate_val * (1.0 - sig))
    return tuple(a.astype(jnp.bfloat16) for a in (gate_cot, grad_val * act, act * up_val))


def exchange_on_device(p, tokens, out_grad, gate_pre, up_pre, hidden_grad):
    T, R, F, bf16 = p.tok, p.rows, p.hidden, jnp.bfloat16
    scratch = [
        pltpu.VMEM((2 * T, F), bf16),
        pltpu.VMEM((4 * T, 2 * F), bf16),
        pltpu.VMEM((2, 4, 4 * T, R), bf16),
        pltpu.VMEM((4, 4, 2 * T, R), bf16),
    ]
    scratch += [pltpu.VMEM(f.shape, bf16) for f in p.flows] * 2
    held = sum(2 * math.prod(ref.shape) for ref in scratch) + 4 * 3 * R * F + 2 * 3 * T * F
    dma = pltpu.SemaphoreType.DMA
    scratch += [dma((7,)), dma((4, 4)), dma((2, 4)), dma((3,)), dma((len(p.flows),))]
    scratch += [dma((f.shape[0] // 2,)) for f in p.flows]
    out = pl.pallas_call(
        functools.partial(exchange_kernel, p),
        out_shape=jax.ShapeDtypeStruct((R, 3 * F), jnp.float32),
        in_specs=[pl.BlockSpec(memory_space=pltpu.HBM)] * 2 + [pl.BlockSpec(memory_space=pltpu.VMEM)] * 3,
        out_specs=pl.BlockSpec(memory_space=pltpu.VMEM),
        scratch_shapes=scratch,
        compiler_params=pltpu.CompilerParams(
            collective_id=0, has_side_effects=True, vmem_limit_bytes=held + SPARE
        ),
    )(tokens, out_grad, *activate(gate_pre, up_pre, hidden_grad))
    return out[:, :F], out[:, F:2 * F], out[:, 2 * F:]


def on_device(n_batch, n_seq, tokens, out_grad, gate_pre, up_pre, hidden_grad):
    tok, width = tokens.shape
    hidden = gate_pre.shape[1]
    sizes = (n_batch, n_seq, tok, width, hidden)
    if Exchange.fits(*sizes):
        return exchange_on_device(
            Exchange(*sizes), tokens, out_grad, gate_pre, up_pre, hidden_grad
        )
    p = Plan(*sizes)
    C, R, bf16 = p.chips, p.rows, jnp.bfloat16
    scratch = [
        pltpu.VMEM((3, 2 * tok, hidden), bf16),
        pltpu.VMEM((2 * tok, 3 * hidden), bf16),
        pltpu.VMEM((p.n_groups, C, 2 * tok, p.block), bf16),
        pltpu.VMEM((p.n_groups, C, 2 * tok, p.block), bf16),
    ]
    sizes = [hi - lo for lo, hi in p.spans]
    scratch += [pltpu.VMEM((n_batch, C, R, size), bf16) for size in sizes]
    for cls, size in enumerate(sizes):
        slots = 1 if p.batch_first[cls] else n_batch
        scratch += [pltpu.VMEM((slots, C >> (j + 1), R, size), bf16) for j in range(p.seq_bits)]
    for cls, size in enumerate(sizes):
        blocks = C if p.batch_first[cls] else 1
        scratch += [pltpu.VMEM((n_batch >> (j + 1), blocks, R, size), bf16) for j in range(p.batch_bits)]
    n_cls = len(sizes)
    dma = pltpu.SemaphoreType.DMA
    scratch += [
        dma((3,)),
        dma((p.n_groups, 2)), dma((p.n_groups, 2)), dma((p.n_groups, 2)),
        dma((n_cls, 2 * p.seq_bits, n_batch)), dma((n_cls, 2 * p.seq_bits, n_batch)),
        dma((n_cls, p.batch_bits, n_batch // 2)), dma((n_cls, p.batch_bits, n_batch // 2)),
    ]
    out = jax.ShapeDtypeStruct((R, hidden), jnp.float32)
    return pl.pallas_call(
        functools.partial(kernel, p),
        out_shape=(out, out, out),
        in_specs=[pl.BlockSpec(memory_space=pltpu.HBM)] * 5,
        out_specs=[pl.BlockSpec(memory_space=pltpu.VMEM)] * 3,
        scratch_shapes=scratch,
        compiler_params=pltpu.CompilerParams(
            collective_id=0, has_side_effects=True, vmem_limit_bytes=67043328
        ),
    )(tokens, out_grad, gate_pre, up_pre, hidden_grad)


def solution(mesh):
    rows = P(("batch", "seq"), None)
    outs = P(("seq", "batch"), None)
    body = functools.partial(on_device, mesh.shape["batch"], mesh.shape["seq"])
    return jax.shard_map(
        body, mesh=mesh, in_specs=(rows,) * 5, out_specs=(outs,) * 3, check_vma=False
    )
```
